256 devices in a mesh: gx: 16 (over z, y_lo), gy: 4 (over x), gz: 4 (over y_hi, core).
Axes of the slice: x: 4, y: 4 (y_hi: 2, y_lo: 2; y = y_hi * 2 + y_lo), z: 8, core: 2. Of those that a mesh axis runs over, the one named last changes fastest.
Arguments:
- pair_map: bfloat16 [1280, 1280, 128], P('gx', ('gy', 'gz')), may hold values from -6 to 6
- residue_mask: int32 [1280], replicated, may hold values 0 or 1
- proj_weight: bfloat16 [128, 512], replicated, may hold values from -0.5 to 0.5
- gate_weight: bfloat16 [128, 128], replicated, may hold values from -0.5 to 0.5
- out_weight: bfloat16 [128, 128], replicated, may hold values from -0.5 to 0.5
Outputs:
- update: bfloat16 [1280, 1280, 128], P('gx', ('gy', 'gz'))
The draws below stay inside these ranges and needn't reach their ends.
All inputs are finite; a program needn't handle non-finite values.
Results may differ from the reference program's by a relative error of at most 0.009.
Values may be sent and summed in bfloat16 or wider, within the bound.
A program may use at most 128 MiB of HBM per device.

```python
import jax
import jax.numpy as jnp
from jax import lax

C = 128
HID = 128
RES_DEV = 80
N = 1280


def touch_ends(result, key, least, top_value):
    dims = result.shape
    place = [jax.random.randint(jax.random.fold_in(key, axis), (), 0, dims[axis]) for axis in range(len(dims))]
    result = result.at[tuple(place)].set(least)
    longest = dims.index(max(dims))
    place[longest] = (place[longest] + 1) % dims[longest]
    return result.at[tuple(place)].set(top_value)


def steps_of(own_key, dims, pieces, smallest, high):
    gain, own = 1.0, jax.random.fold_in(own_key, 6)
    for axis_at, parts in pieces:
        heights = jnp.exp(jax.random.uniform(jax.random.fold_in(own, axis_at), (parts,), jnp.float32, smallest / len(pieces), high / len(pieces)))
        gain = gain * jnp.repeat(heights, dims[axis_at] // parts).reshape([-1 if axis == axis_at else 1 for axis in range(len(dims))])
    return gain


def gaussian(own_key, extent, deviation, bound, pieces=(), kind=jnp.bfloat16):
    entries = deviation * jax.random.normal(own_key, extent, jnp.float32)
    if pieces:
        entries = entries * steps_of(own_key, extent, pieces, -0.22, 0.18)
    return jnp.clip(entries, -bound, bound).astype(kind)


def setup_inputs(seed: int = 0) -> dict:
    splits = jax.random.split(jax.random.key(seed), 6)
    pair_map = gaussian(splits[0], (N, N, C), 1.0, 6.0, ((0, 16), (1, 16)))
    residue_mask = touch_ends((jax.random.randint(splits[1], (N,), 0, 8) < 7).astype(jnp.int32), jax.random.fold_in(splits[1], 1), 0, 1)
    proj_weight = gaussian(splits[2], (C, 4 * HID), C ** -0.5, 0.5)
    gate_weight = gaussian(splits[3], (C, C), C ** -0.5, 0.5)
    out_weight = gaussian(splits[4], (HID, C), HID ** -0.5, 0.5)
    return {"pair_map": pair_map, "residue_mask": residue_mask, "proj_weight": proj_weight, "gate_weight": gate_weight, "out_weight": out_weight}


epsilon = 1.0

def layer_norm(values):
    average = lax.optimization_barrier(jnp.mean(values, axis=-1, keepdims=True))
    centred = values - average
    variance = lax.optimization_barrier(jnp.mean(centred * centred, axis=-1, keepdims=True))
    return centred * lax.rsqrt(variance + epsilon)

def reference(pair_map, residue_mask, proj_weight, gate_weight, out_weight):
    mask_float = residue_mask.astype(jnp.float32)

    def project(inputs):
        row_block, row_mask = inputs
        normed = layer_norm(row_block.astype(jnp.float32)).astype(jnp.bfloat16)
        flattened = normed.reshape(-1, C)
        projected = jnp.dot(flattened, proj_weight, preferred_element_type=jnp.float32).reshape(RES_DEV, N, 4 * HID)
        pair_mask = (row_mask[:, None] * mask_float[None, :])[:, :, None]
        left_proj = (jax.nn.sigmoid(projected[:, :, :HID]) * projected[:, :, HID:2 * HID] * pair_mask).astype(jnp.bfloat16)
        right_proj = (jax.nn.sigmoid(projected[:, :, 2 * HID:3 * HID]) * projected[:, :, 3 * HID:] * pair_mask).astype(jnp.bfloat16)
        gate_value = jax.nn.sigmoid(jnp.dot(flattened, gate_weight, preferred_element_type=jnp.float32)).reshape(RES_DEV, N, C)
        return (left_proj, right_proj, gate_value)
    blocks = pair_map.reshape(N // RES_DEV, RES_DEV, N, C)
    mask_blocks = mask_float.reshape(N // RES_DEV, RES_DEV)
    left_proj, right_proj, gate_value = lax.map(project, (blocks, mask_blocks))
    right_wide = right_proj.reshape(N, N, HID).astype(jnp.float32)

    def finish(inputs):
        left_block, gate_block = inputs
        triangle = jnp.einsum('ikc,jkc->ijc', left_block.astype(jnp.float32), right_wide).astype(jnp.bfloat16)
        normed_tri = layer_norm(triangle.astype(jnp.float32)).astype(jnp.bfloat16)
        mixed_out = jnp.dot(normed_tri.reshape(-1, HID), out_weight, preferred_element_type=jnp.float32).reshape(RES_DEV, N, C)
        return (gate_block * mixed_out).astype(jnp.bfloat16)
    update = lax.map(finish, (left_proj, gate_value))
    return update.reshape(N, N, C)
```

```python
import jax
import jax.numpy as jnp
from jax import lax
from jax.experimental import pallas as pl
from jax.experimental.pallas import tpu as pltpu
from jax.sharding import PartitionSpec as P

MESH = pl.DeviceIdType.MESH
EPS = 1.0
LANES = 128
BLOCK = 80
SUB = 8
SEGS = BLOCK // SUB
TILES = -(-SEGS * BLOCK // LANES)
WIDE = TILES * LANES
CHIPS = 128
BF16 = jnp.bfloat16
F32 = jnp.float32
ANY = pl.BlockSpec(memory_space=pl.ANY)
VMEM = pl.BlockSpec(memory_space=pltpu.VMEM)
BIG = 60 * 2**20


def place():
    gx, gy, gz = lax.axis_index("gx"), lax.axis_index("gy"), lax.axis_index("gz")
    return gy, (gz // 2) * 2 + gx % 2, gx // 2, gz % 2


def device(x, y, z, core):
    return (z * 2 + y % 2, x, (y // 2) * 2 + core)


def layer_norm(values, axis):
    average = jnp.mean(values, axis=axis, keepdims=True)
    centred = values - average
    variance = jnp.mean(centred * centred, axis=axis, keepdims=True)
    return centred * lax.rsqrt(variance + EPS)


def project_kernel(pair_ref, mask_ref, weight_ref, normed_ref, message_ref, left, right):
    def norm_rows(sub, _):
        for seg in range(SEGS):
            rows = pair_ref[SUB * seg + sub].astype(F32)
            normed_ref[sub, pl.ds(seg * BLOCK, BLOCK), :] = layer_norm(rows, -1).astype(BF16)
        normed_ref[sub, pl.ds(SEGS * BLOCK, WIDE - SEGS * BLOCK), :] = jnp.zeros(
            (WIDE - SEGS * BLOCK, LANES), BF16
        )
        for tile in range(TILES):
            block = normed_ref[sub, pl.ds(tile * LANES, LANES), :]
            projected = lax.dot_general(
                weight_ref[...], block, (((1,), (1,)), ((), ())), preferred_element_type=F32
            )
            mask = mask_ref[sub, :, pl.ds(tile * LANES, LANES)]
            first, second, third, fourth = (projected[128 * n : 128 * n + 128] for n in range(4))
            start = tile * SUB + sub
            left[pl.ds(start, CHIPS, stride=TILES * SUB), :] = jax.nn.sigmoid(first) * second * mask
            right[pl.ds(start, CHIPS, stride=TILES * SUB), :] = jax.nn.sigmoid(third) * fourth * mask
        return 0

    lax.fori_loop(0, SUB, norm_rows, 0)

    def pack(channel, _):
        for which, scratch in enumerate((left, right)):
            for tile in range(TILES):
                start = pl.multiple_of((channel * TILES + tile) * SUB, SUB)
                message_ref[channel, which, tile] = scratch[pl.ds(start, SUB), :].astype(BF16)
        return 0

    lax.fori_loop(0, CHIPS, pack, 0)


def project(pair_map, mask, weight):
    return pl.pallas_call(
        project_kernel,
        name="project",
        out_shape=(
            jax.ShapeDtypeStruct((SUB, WIDE, LANES), BF16),
            jax.ShapeDtypeStruct((CHIPS, 2, TILES, SUB, LANES), BF16),
        ),
        in_specs=[VMEM, VMEM, VMEM],
        out_specs=(VMEM, VMEM),
        scratch_shapes=[pltpu.VMEM((CHIPS * TILES * SUB, LANES), F32)] * 2,
        compiler_params=pltpu.CompilerParams(vmem_limit_bytes=BIG),
    )(pair_map, mask, weight)


def spread_kernel(message, arrived, other, send_sem, recv_sem, home_sem, swap_send, swap_recv):
    x, y, z, core = place()
    half = y % 2
    slot = (z * 4 + x) * 4 + (y // 2) * 2 + core

    def send(step, _):
        dz, dx, dy = step % 8, step // 8 % 4, step // 32
        tx, ty, tz = (x + dx) % 4, (y + dy) % 4, (z + dz) % 8
        pltpu.make_async_remote_copy(
            message.at[(tz * 4 + ty) * 4 + tx],
            arrived.at[slot],
            send_sem,
            recv_sem,
            device_id=device(tx, ty, tz, half),
            device_id_type=MESH,
        ).start()
        return 0

    own = message.at[(z * 4 + y) * 4 + x]

    @pl.when(core == half)
    def _():
        pltpu.make_async_copy(own, arrived.at[slot], recv_sem).start()

    @pl.when(core != half)
    def _():
        pltpu.make_async_remote_copy(
            own,
            arrived.at[slot],
            home_sem,
            recv_sem,
            device_id=device(x, y, z, half),
            device_id_type=MESH,
        ).start()

    lax.fori_loop(1, CHIPS, send, 0)
    most = pl.ds(0, CHIPS - 1)
    pltpu.make_async_copy(message.at[most], message.at[most], send_sem).wait()

    @pl.when(core != half)
    def _():
        pltpu.make_async_copy(own, own, home_sem).wait()

    pltpu.make_async_copy(arrived, arrived, recv_sem).wait()
    swap = pltpu.make_async_remote_copy(
        arrived.at[:, 1],
        other,
        swap_send,
        swap_recv,
        device_id=device(x, y, z, 1 - core),
        device_id_type=MESH,
    )
    swap.start()
    swap.wait()


def spread(message):
    return pl.pallas_call(
        spread_kernel,
        name="spread",
        out_shape=(
            jax.ShapeDtypeStruct(message.shape, BF16),
            jax.ShapeDtypeStruct((CHIPS, TILES, SUB, LANES), BF16),
        ),
        in_specs=[ANY],
        out_specs=(ANY, ANY),
        scratch_shapes=[pltpu.SemaphoreType.DMA] * 5,
        compiler_params=pltpu.CompilerParams(has_side_effects=True),
    )(message)


def lane_index():
    return lax.broadcasted_iota(jnp.int32, (SUB, LANES), 1)


def turn(tile, shift):
    shift %= LANES
    return pltpu.roll(tile, shift, 1) if shift else tile


def unpack_into(tiles, target, row, column):
    lanes = lane_index()
    pieces = []
    for seg in range(SEGS):
        first, offset = divmod(seg * BLOCK, LANES)
        piece = turn(tiles[first], -offset)
        if offset + BLOCK > LANES:
            piece = jnp.where(lanes < LANES - offset, piece, turn(tiles[first + 1], -offset))
        pieces.append(jnp.where(lanes < BLOCK, piece, 0.0))
    for pair in range(SEGS // 2):
        both = jnp.concatenate(pieces[2 * pair : 2 * pair + 2], axis=0).astype(BF16)
        target[pl.ds(pl.multiple_of(row + 16 * pair, 16), 16), column] = both


def triangle_kernel(arrived, other, out_ref, left, right, product):
    core = lax.axis_index("gz") % 2
    columns = 16

    def unpack(step, _):
        z, col = step // columns, step % columns
        lanes = pl.ds(pl.multiple_of(col * LANES, LANES), LANES)
        unpack_into(
            [arrived[step, 0, t].astype(F32) for t in range(TILES)], left, z * BLOCK, lanes
        )
        unpack_into(
            [arrived[step, 1, t].astype(F32) for t in range(TILES)],
            right,
            (2 * z + core) * BLOCK,
            lanes,
        )
        unpack_into(
            [other[step, t].astype(F32) for t in range(TILES)],
            right,
            (2 * z + 1 - core) * BLOCK,
            lanes,
        )
        return 0

    lax.fori_loop(0, CHIPS, unpack, 0)
    chunk = 256

    def multiply(step, _):
        start = pl.multiple_of(step * chunk, chunk)
        product[:, pl.ds(start, chunk)] = lax.dot_general(
            left[...],
            right[pl.ds(start, chunk), :],
            (((1,), (1,)), ((), ())),
            preferred_element_type=F32,
        )
        return 0

    lax.fori_loop(0, 1280 // chunk, multiply, 0)

    def pack(step, _):
        z, group = step // 2, step % 2
        lanes = lane_index()
        for seat in range(8):
            low = seat * BLOCK
            tiles = [None] * TILES
            for seg in range(SEGS):
                row = pl.ds(pl.multiple_of(z * BLOCK + seg * SUB, SUB), SUB)
                source = {}

                def lane_tile(number):
                    if number not in source:
                        start = pl.multiple_of(group * 8 * BLOCK + number * LANES, LANES)
                        source[number] = product[row, pl.ds(start, LANES)]
                    return source[number]

                target = seg * BLOCK
                done = 0
                while done < BLOCK:
                    from_tile, from_lane = divmod(low + done, LANES)
                    to_tile, to_lane = divmod(target + done, LANES)
                    run = min(BLOCK - done, LANES - from_lane, LANES - to_lane)
                    piece = turn(lane_tile(from_tile), to_lane - from_lane)
                    if tiles[to_tile] is None:
                        tiles[to_tile] = piece
                    else:
                        tiles[to_tile] = jnp.where(lanes < to_lane, tiles[to_tile], piece)
                    done += run
            for tile in range(TILES):
                out_ref[z * columns + group * 8 + seat, tile] = tiles[tile].astype(BF16)
        return 0

    lax.fori_loop(0, 16, pack, 0)


def triangle(arrived, other):
    return pl.pallas_call(
        triangle_kernel,
        name="triangle",
        out_shape=jax.ShapeDtypeStruct((CHIPS, TILES, SUB, LANES), BF16),
        in_specs=[VMEM, VMEM],
        out_specs=VMEM,
        scratch_shapes=[
            pltpu.VMEM((640, 2048), BF16),
            pltpu.VMEM((1280, 2048), BF16),
            pltpu.VMEM((640, 1280), F32),
        ],
        compiler_params=pltpu.CompilerParams(vmem_limit_bytes=BIG),
    )(arrived, other)


def collect_kernel(blocks, gathered, send_sem, recv_sem):
    x, y, z, core = place()
    channel = (z * 4 + y) * 4 + x

    def send(step, _):
        dz, dx = step % 8, step // 8 % 4
        rest = step // 32
        tz, tx = (z + dz) % 8, (x + dx) % 4
        ty = 2 * ((y // 2 + rest // 2) % 2) + core
        to_core = (core + rest) % 2
        block = blocks.at[(tz * 4 + tx) * 4 + (ty // 2) * 2 + to_core]
        itself = (tz == z) & (tx == x) & (ty == y) & (to_core == core)

        @pl.when(itself)
        def _():
            pltpu.make_async_copy(block, gathered.at[channel], recv_sem).start()

        @pl.when(jnp.logical_not(itself))
        def _():
            pltpu.make_async_remote_copy(
                block,
                gathered.at[channel],
                send_sem,
                recv_sem,
                device_id=device(tx, ty, tz, to_core),
                device_id_type=MESH,
            ).start()

        return 0

    lax.fori_loop(0, CHIPS, send, 0)
    kept = y % 2 == core

    @pl.when(kept)
    def _():
        most = blocks.at[pl.ds(0, CHIPS - 1)]
        pltpu.make_async_copy(most, most, send_sem).wait()

    @pl.when(jnp.logical_not(kept))
    def _():
        pltpu.make_async_copy(blocks, blocks, send_sem).wait()

    pltpu.make_async_copy(gathered, gathered, recv_sem).wait()


def collect(blocks):
    return pl.pallas_call(
        collect_kernel,
        name="collect",
        out_shape=jax.ShapeDtypeStruct(blocks.shape, BF16),
        in_specs=[ANY],
        out_specs=ANY,
        scratch_shapes=[pltpu.SemaphoreType.DMA] * 2,
        compiler_params=pltpu.CompilerParams(has_side_effects=True),
    )(blocks)


def finish_kernel(gathered, normed_ref, gate_weight, out_weight, out_ref, wide, update):
    def widen(channel, _):
        for tile in range(TILES):
            start = pl.multiple_of((channel * TILES + tile) * SUB, SUB)
            wide[pl.ds(start, SUB), :] = gathered[channel, tile].astype(F32)
        return 0

    lax.fori_loop(0, CHIPS, widen, 0)

    def rows_of(sub, _):
        for tile in range(TILES):
            values = wide[pl.ds(tile * SUB + sub, CHIPS, stride=TILES * SUB), :]
            normed_tri = layer_norm(values, 0).astype(BF16)
            mixed = lax.dot_general(
                normed_tri, out_weight[...], (((0,), (0,)), ((), ())), preferred_element_type=F32
            )
            gate = jax.nn.sigmoid(
                jnp.dot(
                    normed_ref[sub, pl.ds(tile * LANES, LANES), :],
                    gate_weight[...],
                    preferred_element_type=F32,
                )
            )
            update[pl.ds(tile * LANES, LANES), :] = (gate * mixed).astype(BF16)
        for seg in range(SEGS):
            out_ref[SUB * seg + sub] = update[pl.ds(seg * BLOCK, BLOCK), :]
        return 0

    lax.fori_loop(0, SUB, rows_of, 0)


def finish(gathered, normed, gate_weight, out_weight):
    return pl.pallas_call(
        finish_kernel,
        name="finish",
        out_shape=jax.ShapeDtypeStruct((BLOCK, BLOCK, LANES), BF16),
        in_specs=[VMEM] * 4,
        out_specs=VMEM,
        scratch_shapes=[
            pltpu.VMEM((CHIPS * TILES * SUB, LANES), F32),
            pltpu.VMEM((WIDE, LANES), BF16),
        ],
        compiler_params=pltpu.CompilerParams(vmem_limit_bytes=BIG),
    )(gathered, normed, gate_weight, out_weight)


def local(pair_map, residue_mask, proj_weight, gate_weight, out_weight):
    mask_float = residue_mask.astype(F32)
    row_mask = lax.dynamic_slice_in_dim(mask_float, lax.axis_index("gx") * BLOCK, BLOCK)
    col = lax.axis_index("gy") * lax.axis_size("gz") + lax.axis_index("gz")
    col_mask = lax.dynamic_slice_in_dim(mask_float, col * BLOCK, BLOCK)
    mask = row_mask.reshape(SEGS, SUB).T[:, :, None] * col_mask[None, None, :]
    mask = jnp.pad(mask.reshape(SUB, 1, SEGS * BLOCK), ((0, 0), (0, 0), (0, WIDE - SEGS * BLOCK)))
    normed, message = project(pair_map, mask, proj_weight.T)
    arrived, other = spread(message)
    blocks = triangle(arrived, other)
    gathered = collect(blocks)
    return finish(gathered, normed, gate_weight, out_weight)


def solution(mesh):
    placed = (P("gx", ("gy", "gz"), None), P(), P(), P(), P())
    return jax.shard_map(
        local, mesh=mesh, in_specs=placed, out_specs=P("gx", ("gy", "gz"), None), check_vma=False
    )
```

```python
import jax
import jax.numpy as jnp
from jax import lax
from jax.experimental import pallas as pl
from jax.experimental.pallas import tpu as pltpu
from jax.sharding import PartitionSpec as P

MESH = pl.DeviceIdType.MESH
EPS = 1.0
LANES = 128
BLOCK = 80
SUB = 8
SEGS = BLOCK // SUB
TILES = -(-SEGS * BLOCK // LANES)
WIDE = TILES * LANES
FLAT = SEGS * BLOCK
BOTH = -(-2 * FLAT // LANES)
EDGE, SPLIT = divmod(FLAT, LANES)
CHIPS = 128
QUARTER = 32
HALF = 640
BF16 = jnp.bfloat16
F32 = jnp.float32
ANY = pl.BlockSpec(memory_space=pl.ANY)
VMEM = pl.BlockSpec(memory_space=pltpu.VMEM)
BIG = 60 * 2**20


def place():
    gx, gy, gz = lax.axis_index("gx"), lax.axis_index("gy"), lax.axis_index("gz")
    return gy, (gz // 2) * 2 + gx % 2, gx // 2, gz % 2


def device(x, y, z, core):
    return (z * 2 + y % 2, x, (y // 2) * 2 + core)


def layer_norm(values, axis):
    average = jnp.mean(values, axis=axis, keepdims=True)
    centred = values - average
    variance = jnp.mean(centred * centred, axis=axis, keepdims=True)
    return centred * lax.rsqrt(variance + EPS)


def lane_index():
    return lax.broadcasted_iota(jnp.int32, (SUB, LANES), 1)


def turn(tile, shift):
    shift %= LANES
    return pltpu.roll(tile, shift, 1) if shift else tile


def unpack_into(tiles, start, target, row, column):
    lanes = lane_index()
    pieces = []
    for seg in range(SEGS):
        first, offset = divmod(start + seg * BLOCK, LANES)
        piece = turn(tiles(first), -offset)
        if offset + BLOCK > LANES:
            piece = jnp.where(lanes < LANES - offset, piece, turn(tiles(first + 1), -offset))
        pieces.append(jnp.where(lanes < BLOCK, piece, 0.0))
    for pair in range(SEGS // 2):
        both = jnp.concatenate(pieces[2 * pair : 2 * pair + 2], axis=0).astype(BF16)
        target[pl.ds(pl.multiple_of(row + 16 * pair, 16), 16), column] = both


def exchange_kernel(
    pair_ref,
    mask_ref,
    weight_ref,
    normed_ref,
    gathered,
    wide,
    message,
    arrived,
    left,
    right,
    other,
    total,
    blocks,
    send_sem,
    home_sem,
    recv_sem,
    swap_send,
    swap_recv,
    back_send,
    back_recv,
):
    x, y, z, core = place()
    half = y % 2
    gx, gy, gz = lax.axis_index("gx"), lax.axis_index("gy"), lax.axis_index("gz")
    barrier = pltpu.get_barrier_semaphore()

    def greet(step, _):
        there = ((gx + step // 16) % 16, (gy + step // 4) % 4, (gz + step) % 4)
        pl.semaphore_signal(barrier, inc=1, device_id=there, device_id_type=MESH)
        return 0

    lax.fori_loop(1, 2 * CHIPS, greet, 0)

    def norm_rows(sub, _):
        for seg in range(SEGS):
            rows = pair_ref[SUB * seg + sub].astype(F32)
            normed_ref[sub, pl.ds(seg * BLOCK, BLOCK), :] = layer_norm(rows, -1).astype(BF16)
        normed_ref[sub, pl.ds(FLAT, WIDE - FLAT), :] = jnp.zeros((WIDE - FLAT, LANES), BF16)
        return 0

    lax.fori_loop(0, SUB, norm_rows, 0)

    def quarter(turn_y, _):
        to_y = (y // 2 + turn_y // 2) % 2 * 2 + (y + turn_y) % 2

        def project(sub, _):
            for tile in range(BOTH):
                if tile < EDGE:
                    block = normed_ref[sub, pl.ds(tile * LANES, LANES), :]
                elif tile == EDGE:
                    block = jnp.concatenate(
                        [
                            normed_ref[sub, pl.ds(EDGE * LANES, SPLIT), :],
                            normed_ref[sub, pl.ds(0, LANES - SPLIT), :],
                        ],
                        axis=0,
                    )
                else:
                    start = (tile - EDGE) * LANES - SPLIT
                    block = normed_ref[sub, pl.ds(start, LANES), :]
                value = None
                for side in range(2):
                    if (side == 0 and tile > EDGE) or (side == 1 and tile < EDGE):
                        continue
                    projected = lax.dot_general(
                        weight_ref[to_y, side],
                        block,
                        (((1,), (1,)), ((), ())),
                        preferred_element_type=F32,
                    )
                    gated = jax.nn.sigmoid(projected[:QUARTER]) * projected[QUARTER:]
                    if value is None:
                        value = gated
                    else:
                        lanes = lax.broadcasted_iota(jnp.int32, (QUARTER, LANES), 1)
                        value = jnp.where(lanes < SPLIT, value, gated)
                mask = mask_ref[sub, :, pl.ds(tile * LANES, LANES)]
                wide[pl.ds(tile * SUB + sub, QUARTER, stride=BOTH * SUB), :] = value * mask
            return 0

        lax.fori_loop(0, SUB, project, 0)

        def pack(number, _):
            for tile in range(BOTH):
                start = pl.multiple_of((number * BOTH + tile) * SUB, SUB)
                message[to_y * QUARTER + number, tile] = wide[pl.ds(start, SUB), :].astype(BF16)
            return 0

        lax.fori_loop(0, QUARTER, pack, 0)

        @pl.when(turn_y == 0)
        def _():
            pl.semaphore_wait(barrier, 2 * CHIPS - 1)
            own = message.at[y * QUARTER + z * 4 + x]
            slot = (x * 4 + (y // 2) * 2 + core) * 8 + z

            @pl.when(core == half)
            def _():
                pltpu.make_async_copy(own, arrived.at[slot], recv_sem.at[0]).start()

            @pl.when(core != half)
            def _():
                pltpu.make_async_remote_copy(
                    own,
                    arrived.at[slot],
                    home_sem,
                    recv_sem.at[0],
                    device_id=device(x, y, z, half),
                    device_id_type=MESH,
                ).start()

        def send(step, _):
            dz, dx = step % 8, step // 8
            tx, tz = (x + dx) % 4, (z + dz) % 8
            pltpu.make_async_remote_copy(
                message.at[to_y * QUARTER + tz * 4 + tx],
                arrived.at[(x * 4 + (y // 2) * 2 + core) * 8 + z],
                send_sem,
                recv_sem.at[turn_y // 2 * 4 + dx],
                device_id=device(tx, to_y, tz, half),
                device_id_type=MESH,
            ).start()
            return 0

        lax.fori_loop(jnp.where(turn_y == 0, 1, 0), QUARTER, send, 0)
        return 0

    lax.fori_loop(0, 4, quarter, 0)

    def clear(step, _):
        total[pl.ds(pl.multiple_of(step * 16, 16), 16), :] = jnp.zeros((16, total.shape[1]), F32)
        return 0

    lax.fori_loop(0, 40, clear, 0)

    def swap_of(group):
        return pltpu.make_async_remote_copy(
            right.at[group],
            other.at[group],
            swap_send.at[group],
            swap_recv.at[group],
            device_id=device(x, y, z, 1 - core),
            device_id_type=MESH,
        )

    def multiply(factor, start):
        total[:, pl.ds(start, HALF)] += lax.dot_general(
            left[...],
            factor[...],
            (((1,), (1,)), ((), ())),
            preferred_element_type=F32,
        )

    def take(group, _):
        base = ((x - group) % 4 * 4 + (y // 2 + group // 4) % 2 * 2) * 8
        some = arrived.at[pl.ds(0, 16)]
        pltpu.make_async_copy(some, some, recv_sem.at[group]).wait()

        def unpack(step, _):
            lanes = pl.ds(pl.multiple_of(step // 8 * LANES, LANES), LANES)
            row = step % 8
            seat = (row // 2 - x) % 4 * 2 + (row - y // 2) % 2

            def tile_of(number):
                return arrived[base + step, number].astype(F32)

            unpack_into(tile_of, FLAT, right.at[group], seat * BLOCK, lanes)
            unpack_into(tile_of, 0, left, row * BLOCK, lanes)
            return 0

        lax.fori_loop(0, 16, unpack, 0)
        swap_of(group).start()
        multiply(right.at[group], 0)
        swap_of(group).wait_recv()
        multiply(other.at[group], HALF)
        return 0

    lax.fori_loop(0, 8, take, 0)

    channel = y * QUARTER + z * 4 + x

    def give(side, _):
        to_core = (core + side) % 2
        for seat in range(8):
            dx, dy = seat // 2, seat % 2
            tx, ty = (x + dx) % 4, 2 * ((y // 2 + dy) % 2) + core

            def one(dz, _, seat=seat, tx=tx, ty=ty):
                tz = (z + dz) % 8
                lanes = lane_index()
                tiles = [None] * TILES
                for seg in range(SEGS):
                    row = pl.ds(pl.multiple_of(tz * BLOCK + seg * SUB, SUB), SUB)
                    low, high, done = seat * BLOCK, seg * BLOCK, 0
                    while done < BLOCK:
                        from_tile, from_lane = divmod(low + done, LANES)
                        to_tile, to_lane = divmod(high + done, LANES)
                        start = pl.multiple_of(side * HALF + from_tile * LANES, LANES)
                        piece = turn(total[row, pl.ds(start, LANES)], to_lane - from_lane)
                        if tiles[to_tile] is None:
                            tiles[to_tile] = piece
                        else:
                            tiles[to_tile] = jnp.where(lanes < to_lane, tiles[to_tile], piece)
                        done += min(BLOCK - done, LANES - from_lane, LANES - to_lane)
                block = blocks.at[(side * 8 + seat) * 8 + dz]
                for tile in range(TILES):
                    block[tile] = tiles[tile].astype(BF16)
                itself = (tz == z) & (tx == x) & (ty == y) & (to_core == core)

                @pl.when(itself)
                def _():
                    pltpu.make_async_copy(block, gathered.at[channel], back_recv).start()

                @pl.when(jnp.logical_not(itself))
                def _():
                    pltpu.make_async_remote_copy(
                        block,
                        gathered.at[channel],
                        back_send,
                        back_recv,
                        device_id=device(tx, ty, tz, to_core),
                        device_id_type=MESH,
                    ).start()

                return 0

            lax.fori_loop(0, 8, one, 0)
        return 0

    lax.fori_loop(0, 2, give, 0)

    most = message.at[pl.ds(0, CHIPS - 1)]
    pltpu.make_async_copy(most, most, send_sem).wait()

    @pl.when(core != half)
    def _():
        pltpu.make_async_copy(message.at[0], message.at[0], home_sem).wait()
        pltpu.make_async_copy(blocks, blocks, back_send).wait()

    @pl.when(core == half)
    def _():
        rest = blocks.at[pl.ds(0, CHIPS - 1)]
        pltpu.make_async_copy(rest, rest, back_send).wait()

    def swapped(group, _):
        swap_of(group).wait_send()
        return 0

    lax.fori_loop(0, 8, swapped, 0)
    pltpu.make_async_copy(gathered, gathered, back_recv).wait()


def exchange(pair_map, mask, weight):
    dma = pltpu.SemaphoreType.DMA
    return pl.pallas_call(
        exchange_kernel,
        name="exchange",
        out_shape=(
            jax.ShapeDtypeStruct((SUB, WIDE, LANES), BF16),
            jax.ShapeDtypeStruct((CHIPS, TILES, SUB, LANES), BF16),
        ),
        in_specs=[VMEM, VMEM, VMEM],
        out_specs=(VMEM, ANY),
        scratch_shapes=[
            pltpu.VMEM((QUARTER * BOTH * SUB, LANES), F32),
            pltpu.VMEM((CHIPS, BOTH, SUB, LANES), BF16),
            pltpu.VMEM((CHIPS, BOTH, SUB, LANES), BF16),
            pltpu.VMEM((HALF, 2 * LANES), BF16),
            pltpu.VMEM((8, HALF, 2 * LANES), BF16),
            pltpu.VMEM((8, HALF, 2 * LANES), BF16),
            pltpu.VMEM((HALF, 2 * HALF), F32),
            pltpu.VMEM((CHIPS, TILES, SUB, LANES), BF16),
            dma,
            dma,
            dma((8,)),
            dma((8,)),
            dma((8,)),
            dma,
            dma,
        ],
        compiler_params=pltpu.CompilerParams(
            vmem_limit_bytes=BIG, has_side_effects=True, collective_id=0
        ),
    )(pair_map, mask, weight)


def finish_kernel(gathered, normed_ref, gate_weight, out_weight, out_ref, wide, update):
    def widen(channel, _):
        for tile in range(TILES):
            start = pl.multiple_of((channel * TILES + tile) * SUB, SUB)
            wide[pl.ds(start, SUB), :] = gathered[channel, tile].astype(F32)
        return 0

    lax.fori_loop(0, CHIPS, widen, 0)

    def rows_of(sub, _):
        for tile in range(TILES):
            values = wide[pl.ds(tile * SUB + sub, CHIPS, stride=TILES * SUB), :]
            normed_tri = layer_norm(values, 0).astype(BF16)
            mixed = lax.dot_general(
                normed_tri, out_weight[...], (((0,), (0,)), ((), ())), preferred_element_type=F32
            )
            gate = jax.nn.sigmoid(
                jnp.dot(
                    normed_ref[sub, pl.ds(tile * LANES, LANES), :],
                    gate_weight[...],
                    preferred_element_type=F32,
                )
            )
            update[pl.ds(tile * LANES, LANES), :] = (gate * mixed).astype(BF16)
        for seg in range(SEGS):
            out_ref[SUB * seg + sub] = update[pl.ds(seg * BLOCK, BLOCK), :]
        return 0

    lax.fori_loop(0, SUB, rows_of, 0)


def finish(gathered, normed, gate_weight, out_weight):
    return pl.pallas_call(
        finish_kernel,
        name="finish",
        out_shape=jax.ShapeDtypeStruct((BLOCK, BLOCK, LANES), BF16),
        in_specs=[VMEM] * 4,
        out_specs=VMEM,
        scratch_shapes=[
            pltpu.VMEM((CHIPS * TILES * SUB, LANES), F32),
            pltpu.VMEM((WIDE, LANES), BF16),
        ],
        compiler_params=pltpu.CompilerParams(vmem_limit_bytes=BIG),
    )(gathered, normed, gate_weight, out_weight)


def local(pair_map, residue_mask, proj_weight, gate_weight, out_weight):
    mask_float = residue_mask.astype(F32)
    row_mask = lax.dynamic_slice_in_dim(mask_float, lax.axis_index("gx") * BLOCK, BLOCK)
    col = lax.axis_index("gy") * lax.axis_size("gz") + lax.axis_index("gz")
    col_mask = lax.dynamic_slice_in_dim(mask_float, col * BLOCK, BLOCK)
    mask = row_mask.reshape(SEGS, SUB).T[:, :, None] * col_mask[None, None, :]
    mask = mask.reshape(SUB, 1, FLAT)
    mask = jnp.pad(jnp.concatenate([mask, mask], axis=2), ((0, 0), (0, 0), (0, BOTH * LANES - 2 * FLAT)))
    weight = proj_weight.T.reshape(2, 2, 4, QUARTER, LANES).transpose(2, 0, 1, 3, 4)
    weight = weight.reshape(4, 2, 2 * QUARTER, LANES)
    normed, gathered = exchange(pair_map, mask, weight)
    return finish(gathered, normed, gate_weight, out_weight)


def solution(mesh):
    placed = (P("gx", ("gy", "gz"), None), P(), P(), P(), P())
    return jax.shard_map(
        local, mesh=mesh, in_specs=placed, out_specs=P("gx", ("gy", "gz"), None), check_vma=False
    )
```

```python
import functools

import jax
import jax.numpy as jnp
from jax import lax
from jax.experimental import pallas as pl
from jax.experimental.pallas import tpu as pltpu
from jax.sharding import PartitionSpec as P

MESH = pl.DeviceIdType.MESH
EPS = 1.0
LANES = 128
BLOCK = 80
FOLD = 4
SUB = 8
SEGS = BLOCK // SUB
TILES = -(-SEGS * BLOCK // LANES)
WIDE = TILES * LANES
EARLY = 5
FLAT = SEGS * BLOCK
BOTH = -(-2 * FLAT // LANES)
EDGE, SPLIT = divmod(FLAT, LANES)
CHIPS = 128
QUARTER = 32
HALF = 640
BF16 = jnp.bfloat16
F32 = jnp.float32
VMEM = pl.BlockSpec(memory_space=pltpu.VMEM)
HBM = pl.BlockSpec(memory_space=pltpu.HBM)
SMEM = pl.BlockSpec(memory_space=pltpu.SMEM)
BIG = 62 * 2**20


def place():
    gx, gy, gz = lax.axis_index("gx"), lax.axis_index("gy"), lax.axis_index("gz")
    return gy, (gz // 2) * 2 + gx % 2, gx // 2, gz % 2


def device(x, y, z, core):
    return (z * 2 + y % 2, x, (y // 2) * 2 + core)


def layer_norm(values, axis):
    average = jnp.mean(values, axis=axis, keepdims=True)
    centred = values - average
    variance = jnp.mean(centred * centred, axis=axis, keepdims=True)
    return centred * lax.rsqrt(variance + EPS)


def lane_index():
    return lax.broadcasted_iota(jnp.int32, (SUB, LANES), 1)


def turn(tile, shift):
    shift %= LANES
    return pltpu.roll(tile, shift, 1) if shift else tile


def unpack_into(tiles, start, target, row, column):
    lanes = lane_index()
    pieces = []
    for seg in range(SEGS):
        first, offset = divmod(start + seg * BLOCK, LANES)
        piece = turn(tiles(first), -offset)
        if offset + BLOCK > LANES:
            piece = jnp.where(lanes < LANES - offset, piece, turn(tiles(first + 1), -offset))
        pieces.append(jnp.where(lanes < BLOCK, piece, 0.0))
    for pair in range(SEGS // 2):
        both = jnp.concatenate(pieces[2 * pair : 2 * pair + 2], axis=0).astype(BF16)
        target[pl.ds(pl.multiple_of(row + 16 * pair, 16), 16), column] = both


def triangle_kernel(
    pair_ref,
    residue_ref,
    proj_ref,
    gate_ref,
    out_weight_ref,
    update_ref,
    raw,
    weight,
    col_mask,
    normed,
    masked,
    gate,
    wide,
    message,
    arrived,
    left,
    right,
    other,
    total,
    early,
    late,
    early_in,
    late_in,
    spread,
    update,
    fetch_sem,
    send_sem,
    home_sem,
    recv_sem,
    swap_send,
    swap_recv,
    back_send,
    back_recv,
):
    x, y, z, core = place()
    half = y % 2
    gx, gy, gz = lax.axis_index("gx"), lax.axis_index("gy"), lax.axis_index("gz")
    barrier = pltpu.get_barrier_semaphore()
    dot = functools.partial(lax.dot_general, preferred_element_type=F32)

    fetch = pltpu.make_async_copy(pair_ref, raw, fetch_sem)
    fetch.start()

    with jax.named_scope("greet"):
        seats_x = [lax.rem(x + n, 4) * 4 for n in range(4)]
        seats_y = [lax.rem(y // 2 + n, 2) * 2 for n in range(2)]
        seats_z = [lax.rem(z + n, 8) * 32 + core * 16 for n in range(8)]
        seats_core = [core, 1 - core]
        for at_z in range(8):
            for at_x in range(4):
                for at_y in range(2):
                    for at_core in range(2):
                        seat = seats_z[at_z] + seats_x[at_x] + seats_y[at_y] + seats_core[at_core]
                        hello = functools.partial(
                            pl.semaphore_signal,
                            barrier,
                            inc=1,
                            device_id=seat,
                            device_id_type=pl.DeviceIdType.LOGICAL,
                        )
                        if at_z or at_x or at_y or at_core:
                            hello()
                        else:
                            pl.when(core != half)(hello)

    with jax.named_scope("masks"):
        for row in range(BLOCK):
            value = residue_ref[(gy * 4 + gz) * BLOCK + row].astype(F32)
            col_mask[pl.ds(row, 1), :] = jnp.full((1, LANES), value)
    mean_of = jnp.full((LANES, LANES), 1.0 / LANES, BF16)

    with jax.named_scope("turn"):
        turned = proj_ref[...].T
        for to_y in range(4):
            for kind in range(4):
                start = kind * LANES + to_y * QUARTER
                target = pl.ds(kind % 2 * QUARTER, QUARTER)
                weight[to_y, kind // 2, target, :] = turned[start : start + QUARTER]
    fetch.wait()

    def norm_rows(sub):
        for seg in range(SEGS):
            row = SUB * seg + sub
            rows = raw[row]
            values = rows.astype(F32)
            average = dot(rows, mean_of, (((1,), (0,)), ((), ())))
            square = jnp.mean(values * values, axis=1, keepdims=True)
            result = (values - average) * lax.rsqrt(square - average * average + EPS)
            normed[sub, pl.ds(seg * BLOCK, BLOCK), :] = result.astype(BF16)
            keep = col_mask[...] * residue_ref[gx * BLOCK + row].astype(F32)
            masked[sub, pl.ds(seg * BLOCK, BLOCK), :] = (result * keep).astype(BF16)
        rest = pl.ds(FLAT, WIDE - FLAT)
        normed[sub, rest, :] = jnp.zeros((WIDE - FLAT, LANES), BF16)
        masked[sub, rest, :] = jnp.zeros((WIDE - FLAT, LANES), BF16)

    def project(sub, to_y):
        if True:
            for tile in range(BOTH):
                if tile < EDGE:
                    block = masked[sub, pl.ds(tile * LANES, LANES), :]
                elif tile == EDGE:
                    block = jnp.concatenate(
                        [
                            masked[sub, pl.ds(EDGE * LANES, SPLIT), :],
                            masked[sub, pl.ds(0, LANES - SPLIT), :],
                        ],
                        axis=0,
                    )
                else:
                    start = (tile - EDGE) * LANES - SPLIT
                    block = masked[sub, pl.ds(start, LANES), :]
                value = None
                for side in range(2):
                    if (side == 0 and tile > EDGE) or (side == 1 and tile < EDGE):
                        continue
                    projected = lax.dot_general(
                        weight[to_y, side],
                        block,
                        (((1,), (1,)), ((), ())),
                        preferred_element_type=F32,
                    )
                    gated = jax.nn.sigmoid(projected[:QUARTER]) * projected[QUARTER:]
                    if value is None:
                        value = gated
                    else:
                        lanes = lax.broadcasted_iota(jnp.int32, (QUARTER, LANES), 1)
                        value = jnp.where(lanes < SPLIT, value, gated)
                wide[pl.ds(tile * SUB + sub, QUARTER, stride=BOTH * SUB), :] = value

    def pack(to_y):
        def one(number, _):
            for tile in range(BOTH):
                start = pl.multiple_of((number * BOTH + tile) * SUB, SUB)
                message[to_y * QUARTER + number, tile] = wide[pl.ds(start, SUB), :].astype(BF16)
            return 0

        with jax.named_scope("pack"):
            lax.fori_loop(0, QUARTER, one, 0)

    slot = (x * 4 + (y // 2) * 2 + core) * 8 + z

    def send_all(turn_y, to_y, first):
        def send(step, _):
            dz, dx = step % 8, step // 8
            tx, tz = (x + dx) % 4, (z + dz) % 8
            pltpu.make_async_remote_copy(
                message.at[to_y * QUARTER + tz * 4 + tx],
                arrived.at[slot],
                send_sem,
                recv_sem.at[turn_y // 2 * 4 + dx],
                device_id=device(tx, to_y, tz, half),
                device_id_type=MESH,
            ).start()
            return 0

        with jax.named_scope("send"):
            lax.fori_loop(first, QUARTER, send, 0)

    with jax.named_scope("norm"):
        for sub in range(SUB):
            norm_rows(sub)
            project(sub, y)
    pack(y)
    with jax.named_scope("meet"):

        @pl.when(core == half)
        def _():
            pl.semaphore_wait(barrier, CHIPS - 1)

        @pl.when(core != half)
        def _():
            pl.semaphore_wait(barrier, CHIPS)

    own = message.at[y * QUARTER + z * 4 + x]

    @pl.when(core == half)
    def _():
        pltpu.make_async_copy(own, arrived.at[slot], recv_sem.at[0]).start()

    @pl.when(core != half)
    def _():
        pltpu.make_async_remote_copy(
            own,
            arrived.at[slot],
            home_sem,
            recv_sem.at[0],
            device_id=device(x, y, z, half),
            device_id_type=MESH,
        ).start()

    send_all(0, y, 1)

    def quarter(turn_y, _):
        to_y = (y // 2 + turn_y // 2) % 2 * 2 + (y + turn_y) % 2

        def one(sub, _):
            project(sub, to_y)
            return 0

        with jax.named_scope("project"):
            lax.fori_loop(0, SUB, one, 0)
        pack(to_y)
        send_all(turn_y, to_y, 0)
        return 0

    lax.fori_loop(1, 4, quarter, 0)

    def gate_rows(sub, _):
        for tile in range(TILES):
            block = normed[sub, pl.ds(tile * LANES, LANES), :]
            value = dot(block, gate_ref[...], (((1,), (0,)), ((), ())))
            gate[sub, pl.ds(tile * LANES, LANES), :] = jax.nn.sigmoid(value)
        return 0

    with jax.named_scope("gate"):
        lax.fori_loop(0, SUB, gate_rows, 0)

    def clear(step, _):
        total[pl.ds(pl.multiple_of(step * 16, 16), 16), :] = jnp.zeros((16, total.shape[1]), F32)
        return 0

    with jax.named_scope("clear"):
        lax.fori_loop(0, 40, clear, 0)

    def swap_of(group):
        return pltpu.make_async_remote_copy(
            right.at[group],
            other.at[group],
            swap_send.at[group],
            swap_recv.at[group],
            device_id=device(x, y, z, 1 - core),
            device_id_type=MESH,
        )

    def multiply(factor, start):
        total[:, pl.ds(start, HALF)] += lax.dot_general(
            left[...],
            factor[...],
            (((1,), (1,)), ((), ())),
            preferred_element_type=F32,
        )

    def take(group):
        base = ((x - group) % 4 * 4 + (y // 2 + group // 4) % 2 * 2) * 8
        some = arrived.at[pl.ds(0, 16)]
        with jax.named_scope("arrive"):
            pltpu.make_async_copy(some, some, recv_sem.at[group]).wait()

        def unpack(source, start, target, row):
            for side in range(2):

                def tile_of(number, side=side):
                    return arrived[base + side * 8 + source, number].astype(F32)

                unpack_into(tile_of, start, target, row * BLOCK, pl.ds(side * LANES, LANES))

        def unpack_right(row, _):
            seat = lax.rem(row // 2 + 4 - x, 4) * 2 + lax.rem(row + y // 2, 2)
            unpack(row, FLAT, right.at[group], seat)
            return 0

        def unpack_left(row, _):
            unpack(row, 0, left, row)
            return 0

        with jax.named_scope("unpack"):
            lax.fori_loop(0, 8, unpack_right, 0)
        swap_of(group).start()
        with jax.named_scope("unpack"):
            lax.fori_loop(0, 8, unpack_left, 0)
        with jax.named_scope("multiply"):
            multiply(right.at[group], 0)

    def take_other(group):
        with jax.named_scope("swap"):
            swap_of(group).wait_recv()
        with jax.named_scope("multiply"):
            multiply(other.at[group], HALF)

    def take_both(group, _):
        take(group)
        take_other(group)
        return 0

    lax.fori_loop(0, 7, take_both, 0)
    take(7)

    channel = y * QUARTER + z * 4 + x

    def launch(side, seat, dz, part):
        tx, tz = lax.rem(x + seat // 2, 4), lax.rem(z + dz, 8)
        ty, to_core = lax.rem(y // 2 + seat % 2, 2), lax.rem(core + side, 2)
        source = (early, late)[part].at[(side * 8 + seat) * 8 + dz]
        target = (early_in, late_in)[part].at[channel]

        def away():
            pltpu.make_async_remote_copy(
                source,
                target,
                back_send.at[part],
                back_recv.at[part],
                device_id=tz * 32 + core * 16 + tx * 4 + ty * 2 + to_core,
                device_id_type=pl.DeviceIdType.LOGICAL,
            ).start()

        def home():
            pltpu.make_async_copy(source, target, back_recv.at[part]).start()

        if seat or side:
            away()
        else:
            itself = (dz == 0) & (core == half)
            pl.when(itself)(home)
            pl.when(jnp.logical_not(itself))(away)

    def give(side):
        for seat in range(8):

            def one(dz, _, seat=seat):
                tz = lax.rem(z + dz, 8)
                lanes = lane_index()
                tiles = [None] * TILES
                for seg in range(SEGS):
                    row = pl.ds(pl.multiple_of(tz * BLOCK + seg * SUB, SUB), SUB)
                    low, high, done = seat * BLOCK, seg * BLOCK, 0
                    while done < BLOCK:
                        from_tile, from_lane = divmod(low + done, LANES)
                        to_tile, to_lane = divmod(high + done, LANES)
                        start = side * HALF + from_tile * LANES
                        piece = turn(total[row, pl.ds(start, LANES)], to_lane - from_lane)
                        if tiles[to_tile] is None:
                            tiles[to_tile] = piece
                        else:
                            tiles[to_tile] = jnp.where(lanes < to_lane, tiles[to_tile], piece)
                        done += min(BLOCK - done, LANES - from_lane, LANES - to_lane)
                number = (side * 8 + seat) * 8 + dz
                for tile in range(EARLY):
                    early[number, tile] = tiles[tile].astype(BF16)
                launch(side, seat, dz, 0)
                folded = turn(pltpu.roll(tiles[EARLY + 1], FOLD, 0), SPLIT)
                folded = jnp.where(lanes < SPLIT, tiles[EARLY + 1], folded)
                late[number, 0] = tiles[EARLY][:FOLD].astype(BF16)
                late[number, 1] = tiles[EARLY][FOLD:].astype(BF16)
                late[number, 2] = folded[:FOLD].astype(BF16)
                return 0

            with jax.named_scope("give"):
                lax.fori_loop(0, 8, one, 0)

    give(0)
    take_other(7)
    give(1)

    def give_late(dz, _):
        for side in range(2):
            for seat in range(8):
                launch(side, seat, dz, 1)
        return 0

    with jax.named_scope("late"):
        lax.fori_loop(0, 8, give_late, 0)

    def whole(rows, count):
        values = spread[pl.ds(rows, CHIPS, stride=count), :]
        normed_tri = layer_norm(values, 0).astype(BF16)
        return dot(normed_tri, out_weight_ref[...], (((0,), (0,)), ((), ())))

    with jax.named_scope("gather"):
        pltpu.make_async_copy(early_in, early_in, back_recv.at[0]).wait()

    def widen_early(number, _):
        for step in range(2):
            for tile in range(EARLY):
                row = pl.multiple_of(((2 * number + step) * EARLY + tile) * SUB, SUB)
                spread[pl.ds(row, SUB), :] = early_in[2 * number + step, tile].astype(F32)
        return 0

    def finish_early(sub, _):
        for tile in range(EARLY):
            mixed = whole(tile * SUB + sub, EARLY * SUB)
            lanes = pl.ds(tile * LANES, LANES)
            update[sub, lanes, :] = (gate[sub, lanes, :] * mixed).astype(BF16)
        return 0

    with jax.named_scope("widen"):
        lax.fori_loop(0, CHIPS // 2, widen_early, 0)
    with jax.named_scope("finish"):
        lax.fori_loop(0, SUB, finish_early, 0)

    with jax.named_scope("gather"):
        pltpu.make_async_copy(late_in, late_in, back_recv.at[1]).wait()

    def widen_late(number, _):
        for step in range(4):
            for tile in range(3):
                row = pl.multiple_of((4 * number + step) * 16, 16) + tile * FOLD
                spread[pl.ds(row, FOLD), :] = late_in[4 * number + step, tile].astype(F32)
        return 0

    with jax.named_scope("widen"):
        lax.fori_loop(0, CHIPS // 4, widen_late, 0)
    with jax.named_scope("finish"):
        for sub in range(SUB):
            mixed = whole(sub, 16)
            lanes = pl.ds(EARLY * LANES, LANES)
            update[sub, lanes, :] = (gate[sub, lanes, :] * mixed).astype(BF16)
        rest = pl.ds((EARLY + 1) * LANES, SPLIT)
        for sub in range(FOLD):
            mixed = whole(SUB + sub, 16)
            update[sub, rest, :] = (gate[sub, rest, :] * mixed[:SPLIT]).astype(BF16)
            update[FOLD + sub, rest, :] = (
                gate[FOLD + sub, rest, :] * mixed[SPLIT : 2 * SPLIT]
            ).astype(BF16)

    def settle(sub, _):
        for seg in range(SEGS):
            update_ref[SUB * seg + sub] = update[sub, pl.ds(seg * BLOCK, BLOCK), :]
        return 0

    with jax.named_scope("settle"):
        lax.fori_loop(0, SUB, settle, 0)
        most = message.at[pl.ds(0, CHIPS - 1)]
        pltpu.make_async_copy(most, most, send_sem).wait()

    for part, source in enumerate((early, late)):

        @pl.when(core != half)
        def _():
            pltpu.make_async_copy(source, source, back_send.at[part]).wait()

        @pl.when(core == half)
        def _():
            rest = source.at[pl.ds(0, CHIPS - 1)]
            pltpu.make_async_copy(rest, rest, back_send.at[part]).wait()

    @pl.when(core != half)
    def _():
        pltpu.make_async_copy(message.at[0], message.at[0], home_sem).wait()

    def swapped(group, _):
        swap_of(group).wait_send()
        return 0

    lax.fori_loop(0, 8, swapped, 0)


def local(pair_map, residue_mask, proj_weight, gate_weight, out_weight):
    dma = pltpu.SemaphoreType.DMA
    return pl.pallas_call(
        triangle_kernel,
        name="triangle",
        out_shape=jax.ShapeDtypeStruct(pair_map.shape, BF16),
        in_specs=[HBM, SMEM, VMEM, VMEM, VMEM],
        out_specs=VMEM,
        scratch_shapes=[
            pltpu.VMEM((BLOCK, BLOCK, LANES), BF16),
            pltpu.VMEM((4, 2, 2 * QUARTER, LANES), BF16),
            pltpu.VMEM((BLOCK, LANES), F32),
            pltpu.VMEM((SUB, WIDE, LANES), BF16),
            pltpu.VMEM((SUB, WIDE, LANES), BF16),
            pltpu.VMEM((SUB, WIDE, LANES), F32),
            pltpu.VMEM((QUARTER * BOTH * SUB, LANES), F32),
            pltpu.VMEM((CHIPS, BOTH, SUB, LANES), BF16),
            pltpu.VMEM((CHIPS, BOTH, SUB, LANES), BF16),
            pltpu.VMEM((HALF, 2 * LANES), BF16),
            pltpu.VMEM((8, HALF, 2 * LANES), BF16),
            pltpu.VMEM((8, HALF, 2 * LANES), BF16),
            pltpu.VMEM((HALF, 2 * HALF), F32),
            pltpu.VMEM((CHIPS, EARLY, SUB, LANES), BF16),
            pltpu.VMEM((CHIPS, 3, FOLD, LANES), BF16),
            pltpu.VMEM((CHIPS, EARLY, SUB, LANES), BF16),
            pltpu.VMEM((CHIPS, 3, FOLD, LANES), BF16),
            pltpu.VMEM((CHIPS * EARLY * SUB, LANES), F32),
            pltpu.VMEM((SUB, WIDE, LANES), BF16),
            dma,
            dma,
            dma,
            dma((8,)),
            dma((8,)),
            dma((8,)),
            dma((2,)),
            dma((2,)),
        ],
        compiler_params=pltpu.CompilerParams(
            vmem_limit_bytes=BIG, has_side_effects=True, collective_id=0
        ),
    )(pair_map, residue_mask, proj_weight, gate_weight, out_weight)


def solution(mesh):
    placed = (P("gx", ("gy", "gz"), None), P(), P(), P(), P())
    return jax.shard_map(
        local, mesh=mesh, in_specs=placed, out_specs=P("gx", ("gy", "gz"), None), check_vma=False
    )
```

```python
import functools

import jax
import jax.numpy as jnp
from jax import lax
from jax.experimental import pallas as pl
from jax.experimental.pallas import tpu as pltpu
from jax.sharding import PartitionSpec as P

MESH = pl.DeviceIdType.MESH
EPS = 1.0
LANES = 128
BLOCK = 80
FOLD = 4
SUB = 8
SEGS = BLOCK // SUB
TILES = -(-SEGS * BLOCK // LANES)
WIDE = TILES * LANES
EARLY = 5
FLAT = SEGS * BLOCK
BOTH = -(-2 * FLAT // LANES)
PACKED = 2 * FLAT * SUB // (FOLD * LANES)
EDGE, SPLIT = divmod(FLAT, LANES)
CHIPS = 128
QUARTER = 32
HALF = 640
BF16 = jnp.bfloat16
F32 = jnp.float32
VMEM = pl.BlockSpec(memory_space=pltpu.VMEM)
HBM = pl.BlockSpec(memory_space=pltpu.HBM)
BIG = 46 * 2**20


def place():
    gx, gy, gz = lax.axis_index("gx"), lax.axis_index("gy"), lax.axis_index("gz")
    return gy, (gz // 2) * 2 + gx % 2, gx // 2, gz % 2


def device(x, y, z, core):
    return (z * 2 + y % 2, x, (y // 2) * 2 + core)


def layer_norm(values, axis):
    average = jnp.mean(values, axis=axis, keepdims=True)
    centred = values - average
    variance = jnp.mean(centred * centred, axis=axis, keepdims=True)
    return centred * lax.rsqrt(variance + EPS)


def lane_index():
    return lax.broadcasted_iota(jnp.int32, (SUB, LANES), 1)


def turn(tile, shift):
    shift %= LANES
    return pltpu.roll(tile, shift, 1) if shift else tile


def unpack_into(tiles, start, target, row, column):
    lanes = lane_index()
    pieces = []
    for seg in range(SEGS):
        first, offset = divmod(start + seg * BLOCK, LANES)
        piece = turn(tiles(first), -offset)
        if offset + BLOCK > LANES:
            piece = jnp.where(lanes < LANES - offset, piece, turn(tiles(first + 1), -offset))
        pieces.append(jnp.where(lanes < BLOCK, piece, 0.0))
    for pair in range(SEGS // 2):
        both = jnp.concatenate(pieces[2 * pair : 2 * pair + 2], axis=0).astype(BF16)
        target[pl.ds(pl.multiple_of(row + 16 * pair, 16), 16), column] = both


def triangle_kernel(
    pair_hbm,
    residue_hbm,
    proj_hbm,
    gate_hbm,
    out_weight_hbm,
    update_ref,
    residue_ref,
    proj_ref,
    gate_ref,
    out_weight_ref,
    raw,
    weight,
    col_mask,
    normed,
    masked,
    gate,
    wide,
    message,
    arrived,
    left,
    right,
    other,
    total,
    early,
    late,
    early_in,
    late_in,
    spread,
    update,
    fetch_sem,
    send_sem,
    home_sem,
    recv_sem,
    swap_send,
    swap_recv,
    back_send,
    back_recv,
):
    x, y, z, core = place()
    half = y % 2
    gx, gy, gz = lax.axis_index("gx"), lax.axis_index("gy"), lax.axis_index("gz")
    barrier = pltpu.get_barrier_semaphore()
    dot = functools.partial(lax.dot_general, preferred_element_type=F32)

    fetches = [
        pltpu.make_async_copy(source, target, fetch_sem.at[number])
        for number, (source, target) in enumerate(
            (
                (pair_hbm, raw),
                (residue_hbm, residue_ref),
                (proj_hbm, proj_ref),
                (gate_hbm, gate_ref),
                (out_weight_hbm, out_weight_ref),
            )
        )
    ]
    for fetch in fetches:
        fetch.start()

    with jax.named_scope("greet"):
        seats_x = [lax.rem(x + n, 4) * 4 for n in range(4)]
        seats_y = [lax.rem(y // 2 + n, 2) * 2 for n in range(2)]
        seats_z = [lax.rem(z + n, 8) * 32 + core * 16 for n in range(8)]
        seats_core = [core, 1 - core]
        for at_z in range(8):
            for at_x in range(4):
                for at_y in range(2):
                    for at_core in range(2):
                        seat = seats_z[at_z] + seats_x[at_x] + seats_y[at_y] + seats_core[at_core]
                        hello = functools.partial(
                            pl.semaphore_signal,
                            barrier,
                            inc=1,
                            device_id=seat,
                            device_id_type=pl.DeviceIdType.LOGICAL,
                        )
                        if at_z or at_x or at_y or at_core:
                            hello()
                        else:
                            pl.when(core != half)(hello)

    for fetch in fetches[1:]:
        fetch.wait()
    with jax.named_scope("masks"):
        for row in range(BLOCK):
            value = residue_ref[(gy * 4 + gz) * BLOCK + row].astype(F32)
            col_mask[pl.ds(row, 1), :] = jnp.full((1, LANES), value)
    mean_of = jnp.full((LANES, LANES), 1.0 / LANES, BF16)

    with jax.named_scope("turn"):
        turned = proj_ref[...].T
        for to_y in range(4):
            for kind in range(4):
                start = kind * LANES + to_y * QUARTER
                target = pl.ds(kind % 2 * QUARTER, QUARTER)
                weight[to_y, kind // 2, target, :] = turned[start : start + QUARTER]
    fetches[0].wait()

    def norm_rows(sub):
        for seg in range(SEGS):
            row = SUB * seg + sub
            rows = raw[row]
            values = rows.astype(F32)
            average = dot(rows, mean_of, (((1,), (0,)), ((), ())))
            square = jnp.mean(values * values, axis=1, keepdims=True)
            result = (values - average) * lax.rsqrt(square - average * average + EPS)
            normed[sub, pl.ds(seg * BLOCK, BLOCK), :] = result.astype(BF16)
            keep = col_mask[...] * residue_ref[gx * BLOCK + row].astype(F32)
            masked[sub, pl.ds(seg * BLOCK, BLOCK), :] = (result * keep).astype(BF16)
        rest = pl.ds(FLAT, WIDE - FLAT)
        normed[sub, rest, :] = jnp.zeros((WIDE - FLAT, LANES), BF16)
        masked[sub, rest, :] = jnp.zeros((WIDE - FLAT, LANES), BF16)

    def project(sub, to_y):
        if True:
            for tile in range(BOTH):
                if tile < EDGE:
                    block = masked[sub, pl.ds(tile * LANES, LANES), :]
                elif tile == EDGE:
                    block = jnp.concatenate(
                        [
                            masked[sub, pl.ds(EDGE * LANES, SPLIT), :],
                            masked[sub, pl.ds(0, LANES - SPLIT), :],
                        ],
                        axis=0,
                    )
                else:
                    start = (tile - EDGE) * LANES - SPLIT
                    block = masked[sub, pl.ds(start, LANES), :]
                value = None
                for side in range(2):
                    if (side == 0 and tile > EDGE) or (side == 1 and tile < EDGE):
                        continue
                    projected = lax.dot_general(
                        weight[to_y, side],
                        block,
                        (((1,), (1,)), ((), ())),
                        preferred_element_type=F32,
                    )
                    gated = jax.nn.sigmoid(projected[:QUARTER]) * projected[QUARTER:]
                    if value is None:
                        value = gated
                    else:
                        lanes = lax.broadcasted_iota(jnp.int32, (QUARTER, LANES), 1)
                        value = jnp.where(lanes < SPLIT, value, gated)
                wide[pl.ds(tile * SUB + sub, QUARTER, stride=BOTH * SUB), :] = value

    def pack(to_y):
        def one(number, _):
            to = to_y * QUARTER + number
            for tile in range(BOTH - 1):
                start = pl.multiple_of((number * BOTH + tile) * SUB, SUB)
                message[to, 2 * tile] = wide[pl.ds(start, FOLD), :].astype(BF16)
                message[to, 2 * tile + 1] = wide[pl.ds(start + FOLD, FOLD), :].astype(BF16)
            last = wide[pl.ds(pl.multiple_of((number * BOTH + BOTH - 1) * SUB, SUB), SUB), :]
            folded = turn(pltpu.roll(last, FOLD, 0), LANES // 2)
            folded = jnp.where(lane_index() < LANES // 2, last, folded)
            message[to, PACKED - 1] = folded[:FOLD].astype(BF16)
            return 0

        with jax.named_scope("pack"):
            lax.fori_loop(0, QUARTER, one, 0)

    slot = (x * 4 + (y // 2) * 2 + core) * 8 + z

    def send_all(turn_y, to_y, first):
        def send(step, _):
            dz, dx = step % 8, step // 8
            tx, tz = (x + dx) % 4, (z + dz) % 8
            pltpu.make_async_remote_copy(
                message.at[to_y * QUARTER + tz * 4 + tx],
                arrived.at[slot],
                send_sem,
                recv_sem.at[turn_y // 2 * 4 + dx],
                device_id=device(tx, to_y, tz, half),
                device_id_type=MESH,
            ).start()
            return 0

        with jax.named_scope("send"):
            lax.fori_loop(first, QUARTER, send, 0)

    with jax.named_scope("norm"):
        for sub in range(SUB):
            norm_rows(sub)
            project(sub, y)
    pack(y)
    with jax.named_scope("meet"):

        @pl.when(core == half)
        def _():
            pl.semaphore_wait(barrier, CHIPS - 1)

        @pl.when(core != half)
        def _():
            pl.semaphore_wait(barrier, CHIPS)

    own = message.at[y * QUARTER + z * 4 + x]

    @pl.when(core == half)
    def _():
        pltpu.make_async_copy(own, arrived.at[slot], recv_sem.at[0]).start()

    @pl.when(core != half)
    def _():
        pltpu.make_async_remote_copy(
            own,
            arrived.at[slot],
            home_sem,
            recv_sem.at[0],
            device_id=device(x, y, z, half),
            device_id_type=MESH,
        ).start()

    send_all(0, y, 1)

    def quarter(turn_y, _):
        to_y = (y // 2 + turn_y // 2) % 2 * 2 + (y + turn_y) % 2

        def one(sub, _):
            project(sub, to_y)
            return 0

        with jax.named_scope("project"):
            lax.fori_loop(0, SUB, one, 0)
        pack(to_y)
        send_all(turn_y, to_y, 0)
        return 0

    lax.fori_loop(1, 4, quarter, 0)

    def gate_rows(sub, _):
        for tile in range(TILES):
            block = normed[sub, pl.ds(tile * LANES, LANES), :]
            value = dot(block, gate_ref[...], (((1,), (0,)), ((), ())))
            gate[sub, pl.ds(tile * LANES, LANES), :] = jax.nn.sigmoid(value)
        return 0

    with jax.named_scope("gate"):
        lax.fori_loop(0, SUB, gate_rows, 0)

    def clear(step, _):
        total[pl.ds(pl.multiple_of(step * 16, 16), 16), :] = jnp.zeros((16, total.shape[1]), F32)
        return 0

    with jax.named_scope("clear"):
        lax.fori_loop(0, 40, clear, 0)

    def swap_of(group):
        return pltpu.make_async_remote_copy(
            right.at[group],
            other.at[group],
            swap_send.at[group],
            swap_recv.at[group],
            device_id=device(x, y, z, 1 - core),
            device_id_type=MESH,
        )

    def multiply(factor, start):
        total[:, pl.ds(start, HALF)] += lax.dot_general(
            left[...],
            factor[...],
            (((1,), (1,)), ((), ())),
            preferred_element_type=F32,
        )

    def take(group):
        base = ((x - group) % 4 * 4 + (y // 2 + group // 4) % 2 * 2) * 8
        some = arrived.at[pl.ds(0, 16)]
        with jax.named_scope("arrive"):
            pltpu.make_async_copy(some, some, recv_sem.at[group]).wait()

        def unpack(source, start, target, row):
            for side in range(2):

                cache = {}

                def tile_of(number, side=side, cache=cache):
                    if number not in cache:
                        at = base + side * 8 + source
                        upper = arrived[at, 2 * number].astype(F32)
                        if number < BOTH - 1:
                            lower = arrived[at, 2 * number + 1].astype(F32)
                        else:
                            lower = turn(upper, LANES // 2)
                        cache[number] = jnp.concatenate([upper, lower], axis=0)
                    return cache[number]

                unpack_into(tile_of, start, target, row * BLOCK, pl.ds(side * LANES, LANES))

        def unpack_right(row, _):
            seat = lax.rem(row // 2 + 4 - x, 4) * 2 + lax.rem(row + y // 2, 2)
            unpack(row, FLAT, right.at[group], seat)
            return 0

        def unpack_left(row, _):
            unpack(row, 0, left, row)
            return 0

        with jax.named_scope("unpack"):
            lax.fori_loop(0, 8, unpack_right, 0)
        swap_of(group).start()
        with jax.named_scope("unpack"):
            lax.fori_loop(0, 8, unpack_left, 0)
        with jax.named_scope("multiply"):
            multiply(right.at[group], 0)

    def take_other(group):
        with jax.named_scope("swap"):
            swap_of(group).wait_recv()
        with jax.named_scope("multiply"):
            multiply(other.at[group], HALF)

    def take_both(group, _):
        take(group)
        take_other(group)
        return 0

    lax.fori_loop(0, 7, take_both, 0)
    take(7)

    channel = y * QUARTER + z * 4 + x

    def launch(side, seat, dz, part):
        tx, tz = lax.rem(x + seat // 2, 4), lax.rem(z + dz, 8)
        ty, to_core = lax.rem(y // 2 + seat % 2, 2), lax.rem(core + side, 2)
        source = (early, late)[part].at[(side * 8 + seat) * 8 + dz]
        target = (early_in, late_in)[part].at[channel]

        def away():
            pltpu.make_async_remote_copy(
                source,
                target,
                back_send.at[part],
                back_recv.at[part],
                device_id=tz * 32 + core * 16 + tx * 4 + ty * 2 + to_core,
                device_id_type=pl.DeviceIdType.LOGICAL,
            ).start()

        def home():
            pltpu.make_async_copy(source, target, back_recv.at[part]).start()

        if seat or side:
            away()
        else:
            itself = (dz == 0) & (core == half)
            pl.when(itself)(home)
            pl.when(jnp.logical_not(itself))(away)

    def give(side):
        for seat in range(8):

            def one(dz, _, seat=seat):
                tz = lax.rem(z + dz, 8)
                lanes = lane_index()
                tiles = [None] * TILES
                for seg in range(SEGS):
                    row = pl.ds(pl.multiple_of(tz * BLOCK + seg * SUB, SUB), SUB)
                    low, high, done = seat * BLOCK, seg * BLOCK, 0
                    while done < BLOCK:
                        from_tile, from_lane = divmod(low + done, LANES)
                        to_tile, to_lane = divmod(high + done, LANES)
                        start = side * HALF + from_tile * LANES
                        piece = turn(total[row, pl.ds(start, LANES)], to_lane - from_lane)
                        if tiles[to_tile] is None:
                            tiles[to_tile] = piece
                        else:
                            tiles[to_tile] = jnp.where(lanes < to_lane, tiles[to_tile], piece)
                        done += min(BLOCK - done, LANES - from_lane, LANES - to_lane)
                number = (side * 8 + seat) * 8 + dz
                for tile in range(EARLY):
                    early[number, tile] = tiles[tile].astype(BF16)
                launch(side, seat, dz, 0)
                folded = turn(pltpu.roll(tiles[EARLY + 1], FOLD, 0), SPLIT)
                folded = jnp.where(lanes < SPLIT, tiles[EARLY + 1], folded)
                late[number, 0] = tiles[EARLY][:FOLD].astype(BF16)
                late[number, 1] = tiles[EARLY][FOLD:].astype(BF16)
                late[number, 2] = folded[:FOLD].astype(BF16)
                return 0

            with jax.named_scope("give"):
                lax.fori_loop(0, 8, one, 0)

    give(0)
    take_other(7)
    give(1)

    def give_late(dz, _):
        for side in range(2):
            for seat in range(8):
                launch(side, seat, dz, 1)
        return 0

    with jax.named_scope("late"):
        lax.fori_loop(0, 8, give_late, 0)

    def whole(rows, count):
        values = spread[pl.ds(rows, CHIPS, stride=count), :]
        normed_tri = layer_norm(values, 0).astype(BF16)
        return dot(normed_tri, out_weight_ref[...], (((0,), (0,)), ((), ())))

    with jax.named_scope("gather"):
        pltpu.make_async_copy(early_in, early_in, back_recv.at[0]).wait()

    def widen_early(number, _):
        for step in range(2):
            for tile in range(EARLY):
                row = pl.multiple_of(((2 * number + step) * EARLY + tile) * SUB, SUB)
                spread[pl.ds(row, SUB), :] = early_in[2 * number + step, tile].astype(F32)
        return 0

    def finish_early(sub, _):
        for tile in range(EARLY):
            mixed = whole(tile * SUB + sub, EARLY * SUB)
            lanes = pl.ds(tile * LANES, LANES)
            update[sub, lanes, :] = (gate[sub, lanes, :] * mixed).astype(BF16)
        return 0

    with jax.named_scope("widen"):
        lax.fori_loop(0, CHIPS // 2, widen_early, 0)
    with jax.named_scope("finish"):
        lax.fori_loop(0, SUB, finish_early, 0)

    with jax.named_scope("gather"):
        pltpu.make_async_copy(late_in, late_in, back_recv.at[1]).wait()

    def widen_late(number, _):
        for step in range(4):
            for tile in range(3):
                row = pl.multiple_of((4 * number + step) * 16, 16) + tile * FOLD
                spread[pl.ds(row, FOLD), :] = late_in[4 * number + step, tile].astype(F32)
        return 0

    with jax.named_scope("widen"):
        lax.fori_loop(0, CHIPS // 4, widen_late, 0)
    with jax.named_scope("finish"):
        for sub in range(SUB):
            mixed = whole(sub, 16)
            lanes = pl.ds(EARLY * LANES, LANES)
            update[sub, lanes, :] = (gate[sub, lanes, :] * mixed).astype(BF16)
        rest = pl.ds((EARLY + 1) * LANES, SPLIT)
        for sub in range(FOLD):
            mixed = whole(SUB + sub, 16)
            update[sub, rest, :] = (gate[sub, rest, :] * mixed[:SPLIT]).astype(BF16)
            update[FOLD + sub, rest, :] = (
                gate[FOLD + sub, rest, :] * mixed[SPLIT : 2 * SPLIT]
            ).astype(BF16)

    def settle(sub, _):
        for seg in range(SEGS):
            update_ref[SUB * seg + sub] = update[sub, pl.ds(seg * BLOCK, BLOCK), :]
        return 0

    with jax.named_scope("settle"):
        lax.fori_loop(0, SUB, settle, 0)
        most = message.at[pl.ds(0, CHIPS - 1)]
        pltpu.make_async_copy(most, most, send_sem).wait()

    for part, source in enumerate((early, late)):

        @pl.when(core != half)
        def _():
            pltpu.make_async_copy(source, source, back_send.at[part]).wait()

        @pl.when(core == half)
        def _():
            rest = source.at[pl.ds(0, CHIPS - 1)]
            pltpu.make_async_copy(rest, rest, back_send.at[part]).wait()

    @pl.when(core != half)
    def _():
        pltpu.make_async_copy(message.at[0], message.at[0], home_sem).wait()

    def swapped(group, _):
        swap_of(group).wait_send()
        return 0

    lax.fori_loop(0, 8, swapped, 0)


def local(pair_map, residue_mask, proj_weight, gate_weight, out_weight):
    dma = pltpu.SemaphoreType.DMA
    inputs = [
        pltpu.with_memory_space_constraint(array, pltpu.HBM)
        for array in (pair_map, residue_mask, proj_weight, gate_weight, out_weight)
    ]
    return pl.pallas_call(
        triangle_kernel,
        name="triangle",
        out_shape=jax.ShapeDtypeStruct(pair_map.shape, BF16),
        in_specs=[HBM] * 5,
        out_specs=VMEM,
        scratch_shapes=[
            pltpu.SMEM(residue_mask.shape, jnp.int32),
            pltpu.VMEM(proj_weight.shape, BF16),
            pltpu.VMEM(gate_weight.shape, BF16),
            pltpu.VMEM(out_weight.shape, BF16),
            pltpu.VMEM((BLOCK, BLOCK, LANES), BF16),
            pltpu.VMEM((4, 2, 2 * QUARTER, LANES), BF16),
            pltpu.VMEM((BLOCK, LANES), F32),
            pltpu.VMEM((SUB, WIDE, LANES), BF16),
            pltpu.VMEM((SUB, WIDE, LANES), BF16),
            pltpu.VMEM((SUB, WIDE, LANES), F32),
            pltpu.VMEM((QUARTER * BOTH * SUB, LANES), F32),
            pltpu.VMEM((CHIPS, PACKED, FOLD, LANES), BF16),
            pltpu.VMEM((CHIPS, PACKED, FOLD, LANES), BF16),
            pltpu.VMEM((HALF, 2 * LANES), BF16),
            pltpu.VMEM((8, HALF, 2 * LANES), BF16),
            pltpu.VMEM((8, HALF, 2 * LANES), BF16),
            pltpu.VMEM((HALF, 2 * HALF), F32),
            pltpu.VMEM((CHIPS, EARLY, SUB, LANES), BF16),
            pltpu.VMEM((CHIPS, 3, FOLD, LANES), BF16),
            pltpu.VMEM((CHIPS, EARLY, SUB, LANES), BF16),
            pltpu.VMEM((CHIPS, 3, FOLD, LANES), BF16),
            pltpu.VMEM((CHIPS * EARLY * SUB, LANES), F32),
            pltpu.VMEM((SUB, WIDE, LANES), BF16),
            dma((5,)),
            dma,
            dma,
            dma((8,)),
            dma((8,)),
            dma((8,)),
            dma((2,)),
            dma((2,)),
        ],
        compiler_params=pltpu.CompilerParams(
            vmem_limit_bytes=BIG, has_side_effects=True, collective_id=0
        ),
    )(*inputs)


def solution(mesh):
    placed = (P("gx", ("gy", "gz"), None), P(), P(), P(), P())
    return jax.shard_map(
        local, mesh=mesh, in_specs=placed, out_specs=P("gx", ("gy", "gz"), None), check_vma=False
    )
```

```python
import functools

import jax
import jax.numpy as jnp
from jax import lax
from jax.experimental import pallas as pl
from jax.experimental.pallas import tpu as pltpu
from jax.sharding import PartitionSpec as P

MESH = pl.DeviceIdType.MESH
EPS = 1.0
LANES = 128
BLOCK = 80
FOLD = 4
SUB = 8
SEGS = BLOCK // SUB
TILES = -(-SEGS * BLOCK // LANES)
WIDE = TILES * LANES
EARLY = 5
FLAT = SEGS * BLOCK
BOTH = -(-2 * FLAT // LANES)
PACKED = 2 * FLAT * SUB // (FOLD * LANES)
EDGE, SPLIT = divmod(FLAT, LANES)
CHIPS = 128
QUARTER = 32
HALF = 640
BF16 = jnp.bfloat16
F32 = jnp.float32
VMEM = pl.BlockSpec(memory_space=pltpu.VMEM)
HBM = pl.BlockSpec(memory_space=pltpu.HBM)
BIG = 46 * 2**20


def place():
    gx, gy, gz = lax.axis_index("gx"), lax.axis_index("gy"), lax.axis_index("gz")
    return gy, (gz // 2) * 2 + gx % 2, gx // 2, gz % 2


def device(x, y, z, core):
    return (z * 2 + y % 2, x, (y // 2) * 2 + core)


def layer_norm(values, axis):
    average = jnp.mean(values, axis=axis, keepdims=True)
    centred = values - average
    variance = jnp.mean(centred * centred, axis=axis, keepdims=True)
    return centred * lax.rsqrt(variance + EPS)


def lane_index():
    return lax.broadcasted_iota(jnp.int32, (SUB, LANES), 1)


def turn(tile, shift):
    shift %= LANES
    return pltpu.roll(tile, shift, 1) if shift else tile


def unpack_into(tiles, start, target, row, column):
    lanes = lane_index()
    pieces = []
    for seg in range(SEGS):
        first, offset = divmod(start + seg * BLOCK, LANES)
        piece = turn(tiles(first), -offset)
        if offset + BLOCK > LANES:
            piece = jnp.where(lanes < LANES - offset, piece, turn(tiles(first + 1), -offset))
        pieces.append(jnp.where(lanes < BLOCK, piece, 0.0))
    for pair in range(SEGS // 2):
        both = jnp.concatenate(pieces[2 * pair : 2 * pair + 2], axis=0).astype(BF16)
        target[pl.ds(pl.multiple_of(row + 16 * pair, 16), 16), column] = both


def triangle_kernel(
    pair_hbm,
    residue_hbm,
    proj_hbm,
    gate_hbm,
    out_weight_hbm,
    update_ref,
    residue_ref,
    proj_ref,
    gate_ref,
    out_weight_ref,
    raw,
    weight,
    col_mask,
    normed,
    masked,
    gate,
    wide,
    message,
    arrived,
    left,
    right,
    other,
    total,
    early,
    late,
    early_in,
    late_in,
    spread,
    update,
    fetch_sem,
    send_sem,
    home_sem,
    recv_sem,
    swap_send,
    swap_recv,
    back_send,
    back_recv,
):
    x, y, z, core = place()
    half = y % 2
    gx, gy, gz = lax.axis_index("gx"), lax.axis_index("gy"), lax.axis_index("gz")
    barrier = pltpu.get_barrier_semaphore()
    dot = functools.partial(lax.dot_general, preferred_element_type=F32)

    fetches = [
        pltpu.make_async_copy(source, target, fetch_sem.at[number])
        for number, (source, target) in enumerate(
            (
                (pair_hbm, raw),
                (residue_hbm, residue_ref),
                (proj_hbm, proj_ref),
                (gate_hbm, gate_ref),
                (out_weight_hbm, out_weight_ref),
            )
        )
    ]
    for fetch in fetches:
        fetch.start()

    with jax.named_scope("greet"):
        seats_x = [lax.rem(x + n, 4) * 4 for n in range(4)]
        seats_y = [lax.rem(y // 2 + n, 2) * 2 for n in range(2)]
        seats_z = [lax.rem(z + n, 8) * 32 + core * 16 for n in range(8)]
        seats_core = [core, 1 - core]
        for at_z in range(8):
            for at_x in range(4):
                for at_y in range(2):
                    for at_core in range(2):
                        seat = seats_z[at_z] + seats_x[at_x] + seats_y[at_y] + seats_core[at_core]
                        hello = functools.partial(
                            pl.semaphore_signal,
                            barrier,
                            inc=1,
                            device_id=seat,
                            device_id_type=pl.DeviceIdType.LOGICAL,
                        )
                        if at_z or at_x or at_y or at_core:
                            hello()
                        else:
                            pl.when(core != half)(hello)

    for fetch in fetches[1:]:
        fetch.wait()
    with jax.named_scope("masks"):
        for row in range(BLOCK):
            value = residue_ref[(gy * 4 + gz) * BLOCK + row].astype(F32)
            col_mask[pl.ds(row, 1), :] = jnp.full((1, LANES), value)
    mean_of = jnp.full((LANES, LANES), 1.0 / LANES, BF16)

    with jax.named_scope("turn"):
        turned = proj_ref[...].T
        for to_y in range(4):
            for kind in range(4):
                start = kind * LANES + to_y * QUARTER
                target = pl.ds(kind % 2 * QUARTER, QUARTER)
                weight[to_y, kind // 2, target, :] = turned[start : start + QUARTER]
    fetches[0].wait()

    def norm_rows(sub):
        for seg in range(SEGS):
            row = SUB * seg + sub
            rows = raw[row]
            values = rows.astype(F32)
            average = dot(rows, mean_of, (((1,), (0,)), ((), ())))
            square = jnp.mean(values * values, axis=1, keepdims=True)
            result = (values - average) * lax.rsqrt(square - average * average + EPS)
            normed[sub, pl.ds(seg * BLOCK, BLOCK), :] = result.astype(BF16)
            keep = col_mask[...] * residue_ref[gx * BLOCK + row].astype(F32)
            masked[sub, pl.ds(seg * BLOCK, BLOCK), :] = (result * keep).astype(BF16)
        rest = pl.ds(FLAT, WIDE - FLAT)
        normed[sub, rest, :] = jnp.zeros((WIDE - FLAT, LANES), BF16)
        masked[sub, rest, :] = jnp.zeros((WIDE - FLAT, LANES), BF16)

    def project(sub, to_y):
        if True:
            for tile in range(BOTH):
                if tile < EDGE:
                    block = masked[sub, pl.ds(tile * LANES, LANES), :]
                elif tile == EDGE:
                    block = jnp.concatenate(
                        [
                            masked[sub, pl.ds(EDGE * LANES, SPLIT), :],
                            masked[sub, pl.ds(0, LANES - SPLIT), :],
                        ],
                        axis=0,
                    )
                else:
                    start = (tile - EDGE) * LANES - SPLIT
                    block = masked[sub, pl.ds(start, LANES), :]
                value = None
                for side in range(2):
                    if (side == 0 and tile > EDGE) or (side == 1 and tile < EDGE):
                        continue
                    projected = lax.dot_general(
                        weight[to_y, side],
                        block,
                        (((1,), (1,)), ((), ())),
                        preferred_element_type=F32,
                    )
                    gated = jax.nn.sigmoid(projected[:QUARTER]) * projected[QUARTER:]
                    if value is None:
                        value = gated
                    else:
                        lanes = lax.broadcasted_iota(jnp.int32, (QUARTER, LANES), 1)
                        value = jnp.where(lanes < SPLIT, value, gated)
                wide[pl.ds(tile * SUB + sub, QUARTER, stride=BOTH * SUB), :] = value

    def pack(to_y):
        def pack_one(number):
            to = to_y * QUARTER + number
            for tile in range(BOTH - 1):
                start = pl.multiple_of((number * BOTH + tile) * SUB, SUB)
                message[to, 2 * tile] = wide[pl.ds(start, FOLD), :].astype(BF16)
                message[to, 2 * tile + 1] = wide[pl.ds(start + FOLD, FOLD), :].astype(BF16)
            last = wide[pl.ds(pl.multiple_of((number * BOTH + BOTH - 1) * SUB, SUB), SUB), :]
            folded = turn(pltpu.roll(last, FOLD, 0), LANES // 2)
            folded = jnp.where(lane_index() < LANES // 2, last, folded)
            message[to, PACKED - 1] = folded[:FOLD].astype(BF16)

        def one(step, _):
            for number in range(8):
                pack_one(8 * step + number)
            return 0

        with jax.named_scope("pack"):
            lax.fori_loop(0, QUARTER // 8, one, 0)

    slot = (x * 4 + (y // 2) * 2 + core) * 8 + z

    def send_all(turn_y, to_y, first):
        def send(step, _):
            dz, dx = step % 8, step // 8
            tx, tz = (x + dx) % 4, (z + dz) % 8
            pltpu.make_async_remote_copy(
                message.at[to_y * QUARTER + tz * 4 + tx],
                arrived.at[slot],
                send_sem,
                recv_sem.at[turn_y // 2 * 4 + dx],
                device_id=device(tx, to_y, tz, half),
                device_id_type=MESH,
            ).start()
            return 0

        with jax.named_scope("send"):
            lax.fori_loop(first, QUARTER, send, 0)

    with jax.named_scope("norm"):
        for sub in range(SUB):
            norm_rows(sub)
            project(sub, y)
    pack(y)
    with jax.named_scope("meet"):

        @pl.when(core == half)
        def _():
            pl.semaphore_wait(barrier, CHIPS - 1)

        @pl.when(core != half)
        def _():
            pl.semaphore_wait(barrier, CHIPS)

    own = message.at[y * QUARTER + z * 4 + x]

    @pl.when(core == half)
    def _():
        pltpu.make_async_copy(own, arrived.at[slot], recv_sem.at[0]).start()

    @pl.when(core != half)
    def _():
        pltpu.make_async_remote_copy(
            own,
            arrived.at[slot],
            home_sem,
            recv_sem.at[0],
            device_id=device(x, y, z, half),
            device_id_type=MESH,
        ).start()

    send_all(0, y, 1)

    def quarter(turn_y, _):
        to_y = (y // 2 + turn_y // 2) % 2 * 2 + (y + turn_y) % 2

        def one(sub, _):
            project(sub, to_y)
            return 0

        with jax.named_scope("project"):
            lax.fori_loop(0, SUB, one, 0)
        pack(to_y)
        send_all(turn_y, to_y, 0)
        return 0

    lax.fori_loop(1, 4, quarter, 0)

    def gate_rows(sub, _):
        for tile in range(TILES):
            block = normed[sub, pl.ds(tile * LANES, LANES), :]
            value = dot(block, gate_ref[...], (((1,), (0,)), ((), ())))
            gate[sub, pl.ds(tile * LANES, LANES), :] = jax.nn.sigmoid(value)
        return 0

    with jax.named_scope("gate"):
        lax.fori_loop(0, SUB, gate_rows, 0)

    def clear(step, _):
        total[pl.ds(pl.multiple_of(step * 16, 16), 16), :] = jnp.zeros((16, total.shape[1]), F32)
        return 0

    with jax.named_scope("clear"):
        lax.fori_loop(0, 40, clear, 0)

    def swap_of(group):
        return pltpu.make_async_remote_copy(
            right.at[group],
            other.at[group],
            swap_send.at[group],
            swap_recv.at[group],
            device_id=device(x, y, z, 1 - core),
            device_id_type=MESH,
        )

    def multiply(group, factor, start):
        total[:, pl.ds(start, HALF)] += lax.dot_general(
            left[group],
            factor[...],
            (((1,), (1,)), ((), ())),
            preferred_element_type=F32,
        )

    def take(group):
        base = ((x - group) % 4 * 4 + (y // 2 + group // 4) % 2 * 2) * 8
        some = arrived.at[pl.ds(0, 16)]
        with jax.named_scope("arrive"):
            pltpu.make_async_copy(some, some, recv_sem.at[group]).wait()

        def unpack(source, start, target, row):
            for side in range(2):

                cache = {}

                def tile_of(number, side=side, cache=cache):
                    if number not in cache:
                        at = base + side * 8 + source
                        upper = arrived[at, 2 * number].astype(F32)
                        if number < BOTH - 1:
                            lower = arrived[at, 2 * number + 1].astype(F32)
                        else:
                            lower = turn(upper, LANES // 2)
                        cache[number] = jnp.concatenate([upper, lower], axis=0)
                    return cache[number]

                unpack_into(tile_of, start, target, row * BLOCK, pl.ds(side * LANES, LANES))

        def unpack_right(step, _):
            for low in range(2):
                seat = lax.rem(step + 4 - x, 4) * 2 + lax.rem(low + y // 2, 2)
                unpack(2 * step + low, FLAT, right.at[group], seat)
            return 0

        def unpack_left(step, _):
            for low in range(2):
                unpack(2 * step + low, 0, left.at[group], 2 * step + low)
            return 0

        with jax.named_scope("unpack"):
            lax.fori_loop(0, 4, unpack_right, 0)
        swap_of(group).start()
        with jax.named_scope("unpack"):
            lax.fori_loop(0, 4, unpack_left, 0)
        with jax.named_scope("multiply"):
            multiply(group, right.at[group], 0)

    def take_other(group):
        with jax.named_scope("swap"):
            swap_of(group).wait_recv()
        with jax.named_scope("multiply"):
            multiply(group, other.at[group], HALF)

    def take_own(group, _):
        take(group)
        pl.when(core != half)(lambda: take_other(group))
        return 0

    lax.fori_loop(0, 7, take_own, 0)
    take(7)

    channel = y * QUARTER + z * 4 + x

    def launch(side, seat, dz, part):
        tx, tz = lax.rem(x + seat // 2, 4), lax.rem(z + dz, 8)
        ty, to_core = lax.rem(y // 2 + seat % 2, 2), lax.rem(core + side, 2)
        source = (early, late)[part].at[(side * 8 + seat) * 8 + dz]
        target = (early_in, late_in)[part].at[channel]

        def away():
            pltpu.make_async_remote_copy(
                source,
                target,
                back_send.at[part],
                back_recv.at[part],
                device_id=tz * 32 + core * 16 + tx * 4 + ty * 2 + to_core,
                device_id_type=pl.DeviceIdType.LOGICAL,
            ).start()

        def home():
            pltpu.make_async_copy(source, target, back_recv.at[part]).start()

        if seat or side:
            away()
        else:
            itself = (dz == 0) & (core == half)
            pl.when(itself)(home)
            pl.when(jnp.logical_not(itself))(away)

    def give(side):
        for seat in range(8):

            def one(dz, _, seat=seat):
                tz = lax.rem(z + dz, 8)
                lanes = lane_index()
                tiles = [None] * TILES
                for seg in range(SEGS):
                    row = pl.ds(pl.multiple_of(tz * BLOCK + seg * SUB, SUB), SUB)
                    low, high, done = seat * BLOCK, seg * BLOCK, 0
                    while done < BLOCK:
                        from_tile, from_lane = divmod(low + done, LANES)
                        to_tile, to_lane = divmod(high + done, LANES)
                        start = side * HALF + from_tile * LANES
                        piece = turn(total[row, pl.ds(start, LANES)], to_lane - from_lane)
                        if tiles[to_tile] is None:
                            tiles[to_tile] = piece
                        else:
                            tiles[to_tile] = jnp.where(lanes < to_lane, tiles[to_tile], piece)
                        done += min(BLOCK - done, LANES - from_lane, LANES - to_lane)
                number = (side * 8 + seat) * 8 + dz
                for tile in range(EARLY):
                    early[number, tile] = tiles[tile].astype(BF16)
                launch(side, seat, dz, 0)
                folded = turn(pltpu.roll(tiles[EARLY + 1], FOLD, 0), SPLIT)
                folded = jnp.where(lanes < SPLIT, tiles[EARLY + 1], folded)
                late[number, 0] = tiles[EARLY][:FOLD].astype(BF16)
                late[number, 1] = tiles[EARLY][FOLD:].astype(BF16)
                late[number, 2] = folded[:FOLD].astype(BF16)
                return 0

            with jax.named_scope("give"):
                lax.fori_loop(0, 8, one, 0)

    give(0)

    @pl.when(core == half)
    def _():
        def rest(group, _):
            take_other(group)
            return 0

        lax.fori_loop(0, 7, rest, 0)

    take_other(7)
    give(1)

    def give_late(dz, _):
        for side in range(2):
            for seat in range(8):
                launch(side, seat, dz, 1)
        return 0

    with jax.named_scope("late"):
        lax.fori_loop(0, 8, give_late, 0)

    def whole(rows, count):
        values = spread[pl.ds(rows, CHIPS, stride=count), :]
        normed_tri = layer_norm(values, 0).astype(BF16)
        return dot(normed_tri, out_weight_ref[...], (((0,), (0,)), ((), ())))

    with jax.named_scope("gather"):
        pltpu.make_async_copy(early_in, early_in, back_recv.at[0]).wait()

    def widen_early(number, _):
        for step in range(2):
            for tile in range(EARLY):
                row = pl.multiple_of(((2 * number + step) * EARLY + tile) * SUB, SUB)
                spread[pl.ds(row, SUB), :] = early_in[2 * number + step, tile].astype(F32)
        return 0

    def finish_early(sub, _):
        for tile in range(EARLY):
            mixed = whole(tile * SUB + sub, EARLY * SUB)
            lanes = pl.ds(tile * LANES, LANES)
            update[sub, lanes, :] = (gate[sub, lanes, :] * mixed).astype(BF16)
        return 0

    with jax.named_scope("widen"):
        lax.fori_loop(0, CHIPS // 2, widen_early, 0)
    with jax.named_scope("finish"):
        lax.fori_loop(0, SUB, finish_early, 0)

    with jax.named_scope("gather"):
        pltpu.make_async_copy(late_in, late_in, back_recv.at[1]).wait()

    def widen_late(number, _):
        for step in range(4):
            for tile in range(3):
                row = pl.multiple_of((4 * number + step) * 16, 16) + tile * FOLD
                spread[pl.ds(row, FOLD), :] = late_in[4 * number + step, tile].astype(F32)
        return 0

    with jax.named_scope("widen"):
        lax.fori_loop(0, CHIPS // 4, widen_late, 0)
    with jax.named_scope("finish"):
        for sub in range(SUB):
            mixed = whole(sub, 16)
            lanes = pl.ds(EARLY * LANES, LANES)
            update[sub, lanes, :] = (gate[sub, lanes, :] * mixed).astype(BF16)
        rest = pl.ds((EARLY + 1) * LANES, SPLIT)
        for sub in range(FOLD):
            mixed = whole(SUB + sub, 16)
            update[sub, rest, :] = (gate[sub, rest, :] * mixed[:SPLIT]).astype(BF16)
            update[FOLD + sub, rest, :] = (
                gate[FOLD + sub, rest, :] * mixed[SPLIT : 2 * SPLIT]
            ).astype(BF16)

    def settle(sub, _):
        for seg in range(SEGS):
            update_ref[SUB * seg + sub] = update[sub, pl.ds(seg * BLOCK, BLOCK), :]
        return 0

    with jax.named_scope("settle"):
        lax.fori_loop(0, SUB, settle, 0)
        most = message.at[pl.ds(0, CHIPS - 1)]
        pltpu.make_async_copy(most, most, send_sem).wait()

    for part, source in enumerate((early, late)):

        @pl.when(core != half)
        def _():
            pltpu.make_async_copy(source, source, back_send.at[part]).wait()

        @pl.when(core == half)
        def _():
            rest = source.at[pl.ds(0, CHIPS - 1)]
            pltpu.make_async_copy(rest, rest, back_send.at[part]).wait()

    @pl.when(core != half)
    def _():
        pltpu.make_async_copy(message.at[0], message.at[0], home_sem).wait()

    def swapped(group, _):
        swap_of(group).wait_send()
        return 0

    lax.fori_loop(0, 8, swapped, 0)


def local(pair_map, residue_mask, proj_weight, gate_weight, out_weight):
    dma = pltpu.SemaphoreType.DMA
    inputs = [
        pltpu.with_memory_space_constraint(array, pltpu.HBM)
        for array in (pair_map, residue_mask, proj_weight, gate_weight, out_weight)
    ]
    return pl.pallas_call(
        triangle_kernel,
        name="triangle",
        out_shape=jax.ShapeDtypeStruct(pair_map.shape, BF16),
        in_specs=[HBM] * 5,
        out_specs=VMEM,
        scratch_shapes=[
            pltpu.SMEM(residue_mask.shape, jnp.int32),
            pltpu.VMEM(proj_weight.shape, BF16),
            pltpu.VMEM(gate_weight.shape, BF16),
            pltpu.VMEM(out_weight.shape, BF16),
            pltpu.VMEM((BLOCK, BLOCK, LANES), BF16),
            pltpu.VMEM((4, 2, 2 * QUARTER, LANES), BF16),
            pltpu.VMEM((BLOCK, LANES), F32),
            pltpu.VMEM((SUB, WIDE, LANES), BF16),
            pltpu.VMEM((SUB, WIDE, LANES), BF16),
            pltpu.VMEM((SUB, WIDE, LANES), F32),
            pltpu.VMEM((QUARTER * BOTH * SUB, LANES), F32),
            pltpu.VMEM((CHIPS, PACKED, FOLD, LANES), BF16),
            pltpu.VMEM((CHIPS, PACKED, FOLD, LANES), BF16),
            pltpu.VMEM((8, HALF, 2 * LANES), BF16),
            pltpu.VMEM((8, HALF, 2 * LANES), BF16),
            pltpu.VMEM((8, HALF, 2 * LANES), BF16),
            pltpu.VMEM((HALF, 2 * HALF), F32),
            pltpu.VMEM((CHIPS, EARLY, SUB, LANES), BF16),
            pltpu.VMEM((CHIPS, 3, FOLD, LANES), BF16),
            pltpu.VMEM((CHIPS, EARLY, SUB, LANES), BF16),
            pltpu.VMEM((CHIPS, 3, FOLD, LANES), BF16),
            pltpu.VMEM((CHIPS * EARLY * SUB, LANES), F32),
            pltpu.VMEM((SUB, WIDE, LANES), BF16),
            dma((5,)),
            dma,
            dma,
            dma((8,)),
            dma((8,)),
            dma((8,)),
            dma((2,)),
            dma((2,)),
        ],
        compiler_params=pltpu.CompilerParams(
            vmem_limit_bytes=BIG, has_side_effects=True, collective_id=0
        ),
    )(*inputs)


def solution(mesh):
    placed = (P("gx", ("gy", "gz"), None), P(), P(), P(), P())
    return jax.shard_map(
        local, mesh=mesh, in_specs=placed, out_specs=P("gx", ("gy", "gz"), None), check_vma=False
    )
```

```python
import functools

import jax
import jax.numpy as jnp
from jax import lax
from jax.experimental import pallas as pl
from jax.experimental.pallas import tpu as pltpu
from jax.sharding import PartitionSpec as P

MESH = pl.DeviceIdType.MESH
EPS = 1.0
LANES = 128
BLOCK = 80
FOLD = 4
SUB = 8
SEGS = BLOCK // SUB
TILES = -(-SEGS * BLOCK // LANES)
WIDE = TILES * LANES
EARLY = 5
FLAT = SEGS * BLOCK
BOTH = -(-2 * FLAT // LANES)
PACKED = 2 * FLAT * SUB // (FOLD * LANES)
EDGE, SPLIT = divmod(FLAT, LANES)
CHIPS = 128
QUARTER = 32
HALF = 640
BF16 = jnp.bfloat16
F32 = jnp.float32
VMEM = pl.BlockSpec(memory_space=pltpu.VMEM)
HBM = pl.BlockSpec(memory_space=pltpu.HBM)
BIG = 46 * 2**20


def place():
    gx, gy, gz = lax.axis_index("gx"), lax.axis_index("gy"), lax.axis_index("gz")
    return gy, (gz // 2) * 2 + gx % 2, gx // 2, gz % 2


def device(x, y, z, core):
    return (z * 2 + y % 2, x, (y // 2) * 2 + core)


def far_first(step):
    half = (step + 1) // 2
    return 4 + half * (1 - 2 * lax.rem(step, 2))


def layer_norm(values, axis):
    average = jnp.mean(values, axis=axis, keepdims=True)
    centred = values - average
    variance = jnp.mean(centred * centred, axis=axis, keepdims=True)
    return centred * lax.rsqrt(variance + EPS)


def lane_index():
    return lax.broadcasted_iota(jnp.int32, (SUB, LANES), 1)


def turn(tile, shift):
    shift %= LANES
    return pltpu.roll(tile, shift, 1) if shift else tile


def unpack_into(tiles, start, target, row, column):
    lanes = lane_index()
    pieces = []
    for seg in range(SEGS):
        first, offset = divmod(start + seg * BLOCK, LANES)
        piece = turn(tiles(first), -offset)
        if offset + BLOCK > LANES:
            piece = jnp.where(lanes < LANES - offset, piece, turn(tiles(first + 1), -offset))
        pieces.append(jnp.where(lanes < BLOCK, piece, 0.0))
    for pair in range(SEGS // 2):
        both = jnp.concatenate(pieces[2 * pair : 2 * pair + 2], axis=0).astype(BF16)
        target[pl.ds(pl.multiple_of(row + 16 * pair, 16), 16), column] = both


def triangle_kernel(
    pair_hbm,
    residue_hbm,
    proj_hbm,
    gate_hbm,
    out_weight_hbm,
    update_ref,
    residue_ref,
    proj_ref,
    gate_ref,
    out_weight_ref,
    raw,
    weight,
    col_mask,
    normed,
    masked,
    gate,
    wide,
    message,
    arrived,
    left,
    right,
    other,
    total,
    early,
    late,
    early_in,
    late_in,
    spread,
    update,
    fetch_sem,
    send_sem,
    home_sem,
    recv_sem,
    swap_send,
    swap_recv,
    back_send,
    back_recv,
):
    x, y, z, core = place()
    half = y % 2
    gx, gy, gz = lax.axis_index("gx"), lax.axis_index("gy"), lax.axis_index("gz")
    barrier = pltpu.get_barrier_semaphore()
    dot = functools.partial(lax.dot_general, preferred_element_type=F32)

    fetches = [
        pltpu.make_async_copy(source, target, fetch_sem.at[number])
        for number, (source, target) in enumerate(
            (
                (pair_hbm, raw),
                (residue_hbm, residue_ref),
                (proj_hbm, proj_ref),
                (gate_hbm, gate_ref),
                (out_weight_hbm, out_weight_ref),
            )
        )
    ]
    for fetch in fetches:
        fetch.start()

    with jax.named_scope("greet"):
        seats_x = [lax.rem(x + n, 4) * 4 for n in range(4)]
        seats_y = [lax.rem(y // 2 + n, 2) * 2 for n in range(2)]
        seats_z = [lax.rem(z + n, 8) * 32 + core * 16 for n in range(8)]
        seats_core = [core, 1 - core]
        for at_z in range(8):
            for at_x in range(4):
                for at_y in range(2):
                    for at_core in range(2):
                        seat = seats_z[at_z] + seats_x[at_x] + seats_y[at_y] + seats_core[at_core]
                        hello = functools.partial(
                            pl.semaphore_signal,
                            barrier,
                            inc=1,
                            device_id=seat,
                            device_id_type=pl.DeviceIdType.LOGICAL,
                        )
                        if at_z or at_x or at_y or at_core:
                            hello()
                        else:
                            pl.when(core != half)(hello)

    for fetch in fetches[1:]:
        fetch.wait()
    with jax.named_scope("masks"):
        for row in range(BLOCK):
            value = residue_ref[(gy * 4 + gz) * BLOCK + row].astype(F32)
            col_mask[pl.ds(row, 1), :] = jnp.full((1, LANES), value)
    mean_of = jnp.full((LANES, LANES), 1.0 / LANES, BF16)

    with jax.named_scope("turn"):
        turned = proj_ref[...].T
        for to_y in range(4):
            for kind in range(4):
                start = kind * LANES + to_y * QUARTER
                target = pl.ds(kind % 2 * QUARTER, QUARTER)
                weight[to_y, kind // 2, target, :] = turned[start : start + QUARTER]
    fetches[0].wait()

    def norm_rows(sub):
        for seg in range(SEGS):
            row = SUB * seg + sub
            rows = raw[row]
            values = rows.astype(F32)
            average = dot(rows, mean_of, (((1,), (0,)), ((), ())))
            square = jnp.mean(values * values, axis=1, keepdims=True)
            result = (values - average) * lax.rsqrt(square - average * average + EPS)
            normed[sub, pl.ds(seg * BLOCK, BLOCK), :] = result.astype(BF16)
            keep = col_mask[...] * residue_ref[gx * BLOCK + row].astype(F32)
            masked[sub, pl.ds(seg * BLOCK, BLOCK), :] = (result * keep).astype(BF16)
        rest = pl.ds(FLAT, WIDE - FLAT)
        normed[sub, rest, :] = jnp.zeros((WIDE - FLAT, LANES), BF16)
        masked[sub, rest, :] = jnp.zeros((WIDE - FLAT, LANES), BF16)

    def project(sub, to_y):
        if True:
            for tile in range(BOTH):
                if tile < EDGE:
                    block = masked[sub, pl.ds(tile * LANES, LANES), :]
                elif tile == EDGE:
                    block = jnp.concatenate(
                        [
                            masked[sub, pl.ds(EDGE * LANES, SPLIT), :],
                            masked[sub, pl.ds(0, LANES - SPLIT), :],
                        ],
                        axis=0,
                    )
                else:
                    start = (tile - EDGE) * LANES - SPLIT
                    block = masked[sub, pl.ds(start, LANES), :]
                value = None
                for side in range(2):
                    if (side == 0 and tile > EDGE) or (side == 1 and tile < EDGE):
                        continue
                    projected = lax.dot_general(
                        weight[to_y, side],
                        block,
                        (((1,), (1,)), ((), ())),
                        preferred_element_type=F32,
                    )
                    gated = jax.nn.sigmoid(projected[:QUARTER]) * projected[QUARTER:]
                    if value is None:
                        value = gated
                    else:
                        lanes = lax.broadcasted_iota(jnp.int32, (QUARTER, LANES), 1)
                        value = jnp.where(lanes < SPLIT, value, gated)
                wide[pl.ds(tile * SUB + sub, QUARTER, stride=BOTH * SUB), :] = value

    def pack(to_y):
        def pack_one(number):
            to = to_y * QUARTER + number
            for tile in range(BOTH - 1):
                start = pl.multiple_of((number * BOTH + tile) * SUB, SUB)
                message[to, 2 * tile] = wide[pl.ds(start, FOLD), :].astype(BF16)
                message[to, 2 * tile + 1] = wide[pl.ds(start + FOLD, FOLD), :].astype(BF16)
            last = wide[pl.ds(pl.multiple_of((number * BOTH + BOTH - 1) * SUB, SUB), SUB), :]
            folded = turn(pltpu.roll(last, FOLD, 0), LANES // 2)
            folded = jnp.where(lane_index() < LANES // 2, last, folded)
            message[to, PACKED - 1] = folded[:FOLD].astype(BF16)

        def one(step, _):
            for number in range(8):
                pack_one(8 * step + number)
            return 0

        with jax.named_scope("pack"):
            lax.fori_loop(0, QUARTER // 8, one, 0)

    slot = (x * 4 + (y // 2) * 2 + core) * 8 + z

    def send_all(turn_y, to_y, first, order):
        def send(step, _):
            dz, dx = lax.rem(step, 8), step // 8
            if order:
                dz = order(dz)
            tx, tz = lax.rem(x + dx, 4), lax.rem(z + dz, 8)
            pltpu.make_async_remote_copy(
                message.at[to_y * QUARTER + tz * 4 + tx],
                arrived.at[slot],
                send_sem,
                recv_sem.at[turn_y // 2 * 4 + dx],
                device_id=device(tx, to_y, tz, half),
                device_id_type=MESH,
            ).start()
            return 0

        with jax.named_scope("send"):
            lax.fori_loop(first, QUARTER, send, 0)

    with jax.named_scope("norm"):
        for sub in range(SUB):
            norm_rows(sub)
            project(sub, y)
    pack(y)
    with jax.named_scope("meet"):

        @pl.when(core == half)
        def _():
            pl.semaphore_wait(barrier, CHIPS - 1)

        @pl.when(core != half)
        def _():
            pl.semaphore_wait(barrier, CHIPS)

    own = message.at[y * QUARTER + z * 4 + x]

    @pl.when(core == half)
    def _():
        pltpu.make_async_copy(own, arrived.at[slot], recv_sem.at[0]).start()

    @pl.when(core != half)
    def _():
        pltpu.make_async_remote_copy(
            own,
            arrived.at[slot],
            home_sem,
            recv_sem.at[0],
            device_id=device(x, y, z, half),
            device_id_type=MESH,
        ).start()

    send_all(0, y, 1, None)

    def quarter(turn_y, _):
        to_y = (y // 2 + turn_y // 2) % 2 * 2 + (y + turn_y) % 2

        def one(sub, _):
            project(sub, to_y)
            return 0

        with jax.named_scope("project"):
            lax.fori_loop(0, SUB, one, 0)
        pack(to_y)
        send_all(turn_y, to_y, 0, far_first)
        return 0

    lax.fori_loop(1, 4, quarter, 0)

    def gate_rows(sub, _):
        for tile in range(TILES):
            block = normed[sub, pl.ds(tile * LANES, LANES), :]
            value = dot(block, gate_ref[...], (((1,), (0,)), ((), ())))
            gate[sub, pl.ds(tile * LANES, LANES), :] = jax.nn.sigmoid(value)
        return 0

    with jax.named_scope("gate"):
        lax.fori_loop(0, SUB, gate_rows, 0)

    def clear(step, _):
        total[pl.ds(pl.multiple_of(step * 16, 16), 16), :] = jnp.zeros((16, total.shape[1]), F32)
        return 0

    with jax.named_scope("clear"):
        lax.fori_loop(0, 40, clear, 0)

    def swap_of(group):
        return pltpu.make_async_remote_copy(
            right.at[group],
            other.at[group],
            swap_send.at[group],
            swap_recv.at[group],
            device_id=device(x, y, z, 1 - core),
            device_id_type=MESH,
        )

    def multiply(group, factor, start):
        total[:, pl.ds(start, HALF)] += lax.dot_general(
            left[group],
            factor[...],
            (((1,), (1,)), ((), ())),
            preferred_element_type=F32,
        )

    def take(group):
        base = ((x - group) % 4 * 4 + (y // 2 + group // 4) % 2 * 2) * 8
        some = arrived.at[pl.ds(0, 16)]
        with jax.named_scope("arrive"):
            pltpu.make_async_copy(some, some, recv_sem.at[group]).wait()

        def unpack(source, start, target, row):
            for side in range(2):

                cache = {}

                def tile_of(number, side=side, cache=cache):
                    if number not in cache:
                        at = base + side * 8 + source
                        upper = arrived[at, 2 * number].astype(F32)
                        if number < BOTH - 1:
                            lower = arrived[at, 2 * number + 1].astype(F32)
                        else:
                            lower = turn(upper, LANES // 2)
                        cache[number] = jnp.concatenate([upper, lower], axis=0)
                    return cache[number]

                unpack_into(tile_of, start, target, row * BLOCK, pl.ds(side * LANES, LANES))

        def unpack_right(step, _):
            for low in range(2):
                seat = lax.rem(step + 4 - x, 4) * 2 + lax.rem(low + y // 2, 2)
                unpack(2 * step + low, FLAT, right.at[group], seat)
            return 0

        def unpack_left(step, _):
            for low in range(2):
                unpack(2 * step + low, 0, left.at[group], 2 * step + low)
            return 0

        with jax.named_scope("unpack"):
            lax.fori_loop(0, 4, unpack_right, 0)
        swap_of(group).start()
        with jax.named_scope("unpack"):
            lax.fori_loop(0, 4, unpack_left, 0)
        with jax.named_scope("multiply"):
            multiply(group, right.at[group], 0)

    def take_other(group):
        with jax.named_scope("swap"):
            swap_of(group).wait_recv()
        with jax.named_scope("multiply"):
            multiply(group, other.at[group], HALF)

    def take_own(group, _):
        take(group)
        pl.when(core != half)(lambda: take_other(group))
        return 0

    lax.fori_loop(0, 7, take_own, 0)
    take(7)

    channel = y * QUARTER + z * 4 + x

    def launch(side, seat, dz, part):
        tx, tz = lax.rem(x + seat // 2, 4), lax.rem(z + dz, 8)
        ty, to_core = lax.rem(y // 2 + seat % 2, 2), lax.rem(core + side, 2)
        source = (early, late)[part].at[(side * 8 + seat) * 8 + dz]
        target = (early_in, late_in)[part].at[channel]

        def away():
            pltpu.make_async_remote_copy(
                source,
                target,
                back_send.at[part],
                back_recv.at[part],
                device_id=tz * 32 + core * 16 + tx * 4 + ty * 2 + to_core,
                device_id_type=pl.DeviceIdType.LOGICAL,
            ).start()

        def home():
            pltpu.make_async_copy(source, target, back_recv.at[part]).start()

        if seat or side:
            away()
        else:
            itself = (dz == 0) & (core == half)
            pl.when(itself)(home)
            pl.when(jnp.logical_not(itself))(away)

    def give(side):
        for seat in range(8):

            def one(step, _, seat=seat):
                dz = far_first(step)
                tz = lax.rem(z + dz, 8)
                lanes = lane_index()
                tiles = [None] * TILES
                for seg in range(SEGS):
                    row = pl.ds(pl.multiple_of(tz * BLOCK + seg * SUB, SUB), SUB)
                    low, high, done = seat * BLOCK, seg * BLOCK, 0
                    while done < BLOCK:
                        from_tile, from_lane = divmod(low + done, LANES)
                        to_tile, to_lane = divmod(high + done, LANES)
                        start = side * HALF + from_tile * LANES
                        piece = turn(total[row, pl.ds(start, LANES)], to_lane - from_lane)
                        if tiles[to_tile] is None:
                            tiles[to_tile] = piece
                        else:
                            tiles[to_tile] = jnp.where(lanes < to_lane, tiles[to_tile], piece)
                        done += min(BLOCK - done, LANES - from_lane, LANES - to_lane)
                number = (side * 8 + seat) * 8 + dz
                for tile in range(EARLY):
                    early[number, tile] = tiles[tile].astype(BF16)
                launch(side, seat, dz, 0)
                folded = turn(pltpu.roll(tiles[EARLY + 1], FOLD, 0), SPLIT)
                folded = jnp.where(lanes < SPLIT, tiles[EARLY + 1], folded)
                late[number, 0] = tiles[EARLY][:FOLD].astype(BF16)
                late[number, 1] = tiles[EARLY][FOLD:].astype(BF16)
                late[number, 2] = folded[:FOLD].astype(BF16)
                return 0

            with jax.named_scope("give"):
                lax.fori_loop(0, 8, one, 0)

    give(0)

    @pl.when(core == half)
    def _():
        def rest(group, _):
            take_other(group)
            return 0

        lax.fori_loop(0, 7, rest, 0)

    take_other(7)
    give(1)

    def give_late(step, _):
        dz = far_first(step)
        for side in range(2):
            for seat in range(8):
                launch(side, seat, dz, 1)
        return 0

    with jax.named_scope("late"):
        lax.fori_loop(0, 8, give_late, 0)

    def whole(rows, count):
        values = spread[pl.ds(rows, CHIPS, stride=count), :]
        normed_tri = layer_norm(values, 0).astype(BF16)
        return dot(normed_tri, out_weight_ref[...], (((0,), (0,)), ((), ())))

    with jax.named_scope("gather"):
        pltpu.make_async_copy(early_in, early_in, back_recv.at[0]).wait()

    def widen_early(number, _):
        for step in range(2):
            for tile in range(EARLY):
                row = pl.multiple_of(((2 * number + step) * EARLY + tile) * SUB, SUB)
                spread[pl.ds(row, SUB), :] = early_in[2 * number + step, tile].astype(F32)
        return 0

    def finish_early(sub, _):
        for tile in range(EARLY):
            mixed = whole(tile * SUB + sub, EARLY * SUB)
            lanes = pl.ds(tile * LANES, LANES)
            update[sub, lanes, :] = (gate[sub, lanes, :] * mixed).astype(BF16)
        return 0

    with jax.named_scope("widen"):
        lax.fori_loop(0, CHIPS // 2, widen_early, 0)
    with jax.named_scope("finish"):
        lax.fori_loop(0, SUB, finish_early, 0)

    with jax.named_scope("gather"):
        pltpu.make_async_copy(late_in, late_in, back_recv.at[1]).wait()

    def widen_late(number, _):
        for step in range(4):
            for tile in range(3):
                row = pl.multiple_of((4 * number + step) * 16, 16) + tile * FOLD
                spread[pl.ds(row, FOLD), :] = late_in[4 * number + step, tile].astype(F32)
        return 0

    with jax.named_scope("widen"):
        lax.fori_loop(0, CHIPS // 4, widen_late, 0)
    with jax.named_scope("finish"):
        for sub in range(SUB):
            mixed = whole(sub, 16)
            lanes = pl.ds(EARLY * LANES, LANES)
            update[sub, lanes, :] = (gate[sub, lanes, :] * mixed).astype(BF16)
        rest = pl.ds((EARLY + 1) * LANES, SPLIT)
        for sub in range(FOLD):
            mixed = whole(SUB + sub, 16)
            update[sub, rest, :] = (gate[sub, rest, :] * mixed[:SPLIT]).astype(BF16)
            update[FOLD + sub, rest, :] = (
                gate[FOLD + sub, rest, :] * mixed[SPLIT : 2 * SPLIT]
            ).astype(BF16)

    def settle(sub, _):
        for seg in range(SEGS):
            update_ref[SUB * seg + sub] = update[sub, pl.ds(seg * BLOCK, BLOCK), :]
        return 0

    with jax.named_scope("settle"):
        lax.fori_loop(0, SUB, settle, 0)
        most = message.at[pl.ds(0, CHIPS - 1)]
        pltpu.make_async_copy(most, most, send_sem).wait()

    for part, source in enumerate((early, late)):

        @pl.when(core != half)
        def _():
            pltpu.make_async_copy(source, source, back_send.at[part]).wait()

        @pl.when(core == half)
        def _():
            rest = source.at[pl.ds(0, CHIPS - 1)]
            pltpu.make_async_copy(rest, rest, back_send.at[part]).wait()

    @pl.when(core != half)
    def _():
        pltpu.make_async_copy(message.at[0], message.at[0], home_sem).wait()

    def swapped(group, _):
        swap_of(group).wait_send()
        return 0

    lax.fori_loop(0, 8, swapped, 0)


def local(pair_map, residue_mask, proj_weight, gate_weight, out_weight):
    dma = pltpu.SemaphoreType.DMA
    inputs = [
        pltpu.with_memory_space_constraint(array, pltpu.HBM)
        for array in (pair_map, residue_mask, proj_weight, gate_weight, out_weight)
    ]
    return pl.pallas_call(
        triangle_kernel,
        name="triangle",
        out_shape=jax.ShapeDtypeStruct(pair_map.shape, BF16),
        in_specs=[HBM] * 5,
        out_specs=VMEM,
        scratch_shapes=[
            pltpu.SMEM(residue_mask.shape, jnp.int32),
            pltpu.VMEM(proj_weight.shape, BF16),
            pltpu.VMEM(gate_weight.shape, BF16),
            pltpu.VMEM(out_weight.shape, BF16),
            pltpu.VMEM((BLOCK, BLOCK, LANES), BF16),
            pltpu.VMEM((4, 2, 2 * QUARTER, LANES), BF16),
            pltpu.VMEM((BLOCK, LANES), F32),
            pltpu.VMEM((SUB, WIDE, LANES), BF16),
            pltpu.VMEM((SUB, WIDE, LANES), BF16),
            pltpu.VMEM((SUB, WIDE, LANES), F32),
            pltpu.VMEM((QUARTER * BOTH * SUB, LANES), F32),
            pltpu.VMEM((CHIPS, PACKED, FOLD, LANES), BF16),
            pltpu.VMEM((CHIPS, PACKED, FOLD, LANES), BF16),
            pltpu.VMEM((8, HALF, 2 * LANES), BF16),
            pltpu.VMEM((8, HALF, 2 * LANES), BF16),
            pltpu.VMEM((8, HALF, 2 * LANES), BF16),
            pltpu.VMEM((HALF, 2 * HALF), F32),
            pltpu.VMEM((CHIPS, EARLY, SUB, LANES), BF16),
            pltpu.VMEM((CHIPS, 3, FOLD, LANES), BF16),
            pltpu.VMEM((CHIPS, EARLY, SUB, LANES), BF16),
            pltpu.VMEM((CHIPS, 3, FOLD, LANES), BF16),
            pltpu.VMEM((CHIPS * EARLY * SUB, LANES), F32),
            pltpu.VMEM((SUB, WIDE, LANES), BF16),
            dma((5,)),
            dma,
            dma,
            dma((8,)),
            dma((8,)),
            dma((8,)),
            dma((2,)),
            dma((2,)),
        ],
        compiler_params=pltpu.CompilerParams(
            vmem_limit_bytes=BIG, has_side_effects=True, collective_id=0
        ),
    )(*inputs)


def solution(mesh):
    placed = (P("gx", ("gy", "gz"), None), P(), P(), P(), P())
    return jax.shard_map(
        local, mesh=mesh, in_specs=placed, out_specs=P("gx", ("gy", "gz"), None), check_vma=False
    )
```
